32 devices in a mesh: blk: 8 (over y, x, core), inner: 4 (over z).
Axes of the slice: x: 2, y: 2, z: 4, core: 2. Of those that a mesh axis runs over, the one named last changes fastest.
Arguments:
- query_latent: bfloat16 [1024, 16384], P('blk', 'inner'), may hold values from -100 to 100
- query_rotary: bfloat16 [1024, 2048], P('blk', 'inner'), may hold values from -100 to 100
- upstream: bfloat16 [1024, 16384], P('blk', 'inner'), may hold values from -6 to 6
- latent: bfloat16 [1024, 512], P(('blk', 'inner')), may hold values from -8 to 8
- key_rotary: bfloat16 [1024, 64], P(('blk', 'inner')), may hold values from -8 to 8
- pattern: int32 [8, 5], P('blk'), may hold values from -1 to 7, as said below
Outputs:
- query_cotangent: bfloat16 [1024, 16384], P('blk', 'inner')
- rotary_cotangent: bfloat16 [1024, 2048], P('blk', 'inner')
- latent_cotangent: float32 [1024, 512], P(('blk', 'inner'))
- positional_cotangent: float32 [1024, 64], P(('blk', 'inner'))
The draws below stay inside these ranges and needn't reach their ends.
Inputs may be any that keep to these rules, and one draw needn't show every extreme that they name: `pattern`: let d_0 < d_1 < ... be the distinct numbers among 0 to 1 and m * 1 for m = 1 to 4; there are 5 of them. Entry k of row q is either q - d_k or -1, and it is -1 whenever q - d_k < 0. Entry 0 of every row is q.
All inputs are finite; a program needn't handle non-finite values.
Results may differ from the reference program's by a relative error of at most 0.0085.
Values may be sent and summed in bfloat16 or wider, within the bound.
No kernel may reach another device: no remote copies, remote signals or barrier semaphores. Data moves between devices by JAX's collectives and lax.ppermute only.
A program may use at most 128 MiB of HBM per device.

```python
import jax
import jax.numpy as jnp
from jax import lax

HEADS = 32
LATENT = 512
ROPE = 64
NOPE = 128
BLOCK = 128
WIN = 2
NSTR = 4
NB = 8
STRIDE = 1
KMAX = 5
NTOK = 1024


def spacing_draw():
    listed = set(range(WIN))
    for number in range(1, NSTR + 1):
        listed.add(number * STRIDE)
    return sorted(listed)


def key_values(key):
    key_table = jnp.clip(jax.random.normal(jax.random.fold_in(key, 11), (NTOK, LATENT + ROPE), jnp.float32), -6.0, 6.0)
    return key_table


def query_values(key, salt, width):
    values = jnp.clip(jax.random.normal(jax.random.fold_in(key, salt), (NTOK, HEADS, width), jnp.float32), -6.0, 6.0)
    return values.reshape(NTOK, HEADS * width)


def draw_query_latent(key, part):
    return query_values(key, 21, LATENT).astype(jnp.bfloat16)


def draw_query_rotary(key, part):
    return query_values(key, 22, ROPE).astype(jnp.bfloat16)


def draw_latent(key, part):
    key_table = key_values(key)
    return key_table[:, :LATENT].astype(jnp.bfloat16)


def draw_key_rotary(key, part):
    key_table = key_values(key)
    return key_table[:, LATENT:].astype(jnp.bfloat16)


def draw_pattern(key, part):
    spacing = jnp.array(spacing_draw(), dtype=jnp.int32)[None, :]
    picks = jax.random.randint(jax.random.fold_in(key, 31), (NB, KMAX), 0, 2)
    block_rows = jnp.arange(NB, dtype=jnp.int32)[:, None]
    keeping = (spacing < WIN) | (picks == 1)
    inside = block_rows - spacing >= 0
    return jnp.where(keeping & inside, block_rows - spacing, -1).astype(jnp.int32)


def block_levels(own_key, shape, cuts, low, top_value):
    loudness = 1.0
    for axis_at, shards_of in cuts:
        heights = jax.random.uniform(jax.random.fold_in(jax.random.fold_in(own_key, 6), axis_at), (shards_of,), jnp.float32, low / len(cuts), top_value / len(cuts))
        loudness = loudness * jnp.repeat(jnp.exp(heights), shape[axis_at] // shards_of).reshape((-1,) + (1,) * (len(shape) - 1 - axis_at))
    return loudness


def centred(key, shape, spread, bound, split=(), kind=jnp.bfloat16):
    result = jax.random.normal(key, shape, jnp.float32) * spread
    if len(split) > 0:
        result = block_levels(key, shape, split, -0.22, 0.18) * result
    return jnp.clip(result, min=-bound, max=bound).astype(kind)


def setup_inputs(seed: int = 0) -> dict:
    key_list = jax.random.split(jax.random.key(seed), 7)
    query_latent = draw_query_latent(jax.random.fold_in(key_list[6], 71), 0)
    query_rotary = draw_query_rotary(jax.random.fold_in(key_list[6], 71), 0)
    upstream = centred(key_list[2], (NTOK, HEADS * LATENT), 1.0, 6.0, ((0, 8), (1, 4)))
    latent = draw_latent(jax.random.fold_in(key_list[6], 71), 0)
    key_rotary = draw_key_rotary(jax.random.fold_in(key_list[6], 71), 0)
    pattern = draw_pattern(jax.random.fold_in(key_list[6], 71), 0)
    return dict(query_latent=query_latent, query_rotary=query_rotary, upstream=upstream, latent=latent, key_rotary=key_rotary, pattern=pattern)


def spacing_list():
    listed = set(range(WIN))
    for number in range(1, NSTR + 1):
        listed.add(number * STRIDE)
    return sorted(listed)


def reference(query_latent, query_rotary, upstream, latent, key_rotary, pattern):
    softmax_scale = (NOPE + ROPE) ** -0.5
    spacing = spacing_list()
    query_blocks = query_latent.reshape(NB, BLOCK, HEADS, LATENT)
    rotary_blocks = query_rotary.reshape(NB, BLOCK, HEADS, ROPE)
    upstream_blocks = upstream.reshape(NB, BLOCK, HEADS, LATENT)
    latent_blocks = latent.reshape(NB, BLOCK, LATENT)
    rotary_keys = key_rotary.reshape(NB, BLOCK, ROPE)
    offsets = jnp.array(spacing, dtype=jnp.int32)
    position = jnp.arange(BLOCK, dtype=jnp.int32)
    causal = position[None, :] <= position[:, None]
    diagonal = offsets == 0

    def one_block(running_state, inputs):
        latent_acc, rotary_acc = running_state
        block_index, query_block, rotary_block, upward, listed = inputs
        sources = jnp.clip(block_index - offsets, 0, NB - 1).astype(jnp.int32)
        key_block = latent_blocks[sources].astype(jnp.float32)
        rope_block = rotary_keys[sources].astype(jnp.float32)
        query_full = query_block.astype(jnp.float32)
        rotary_full = rotary_block.astype(jnp.float32)
        upward_full = upward.astype(jnp.float32)
        scores = (jnp.einsum('thl,kul->thku', query_full, key_block)
                  + jnp.einsum('thr,kur->thku', rotary_full, rope_block)) * softmax_scale
        allowed = (listed >= 0)[None, None, :, None] & (causal[:, None, None, :] | ~diagonal[None, None, :, None])
        scores = jnp.where(allowed, scores, -jnp.inf)
        row_peak = jnp.max(scores, axis=(2, 3))
        log_total = row_peak + jnp.log(jnp.sum(jnp.exp(scores - row_peak[:, :, None, None]), axis=(2, 3)))
        weights = jnp.where(allowed, jnp.exp(scores - log_total[:, :, None, None]), 0.0)
        dprobs = jnp.einsum('thl,kul->thku', upward_full, key_block)
        correction = jnp.sum(weights * dprobs, axis=(2, 3))
        dscores = weights * (dprobs - correction[:, :, None, None])
        query_cot = (softmax_scale * jnp.einsum('thku,kul->thl', dscores, key_block)).astype(jnp.bfloat16)
        rotary_cot = (softmax_scale * jnp.einsum('thku,kur->thr', dscores, rope_block)).astype(jnp.bfloat16)
        key_part = (softmax_scale * jnp.einsum('thku,thl->kul', dscores, query_full)
                    + jnp.einsum('thku,thl->kul', weights, upward_full))
        rope_part = softmax_scale * jnp.einsum('thku,thr->kur', dscores, rotary_full)
        latent_acc = latent_acc.at[sources].add(key_part)
        rotary_acc = rotary_acc.at[sources].add(rope_part)
        return (latent_acc, rotary_acc), (query_cot, rotary_cot)

    initial = (jnp.zeros((NB, BLOCK, LATENT), jnp.float32), jnp.zeros((NB, BLOCK, ROPE), jnp.float32))
    block_ids = jnp.arange(NB, dtype=jnp.int32)
    (latent_acc, rotary_acc), (query_cot, rotary_cot) = lax.scan(
        one_block, initial, (block_ids, query_blocks, rotary_blocks, upstream_blocks, pattern))
    return (query_cot.reshape(NTOK, HEADS * LATENT), rotary_cot.reshape(NTOK, HEADS * ROPE),
            latent_acc.reshape(NTOK, LATENT), rotary_acc.reshape(NTOK, ROPE))
```

```python
import functools

import jax
import jax.numpy as jnp
from jax import lax
from jax.experimental import pallas as pl
from jax.experimental.pallas import tpu as pltpu
from jax.sharding import PartitionSpec as P

NOPE = 128
WIN = 2
NSTR = 4
LOG2E = 1.4426950408889634
BF16 = jnp.bfloat16
F32 = jnp.float32


def spacing_list(blocks):
    spacing = blocks // 8
    listed = set(range(WIN))
    for number in range(1, NSTR + 1):
        listed.add(number * spacing)
    return sorted(listed)


def rotated(value, axis, steps):
    count = lax.axis_size(axis)
    return lax.ppermute(value, axis, [(s, (s + steps) % count) for s in range(count)])


def stacked_pair(pair, width):
    return jnp.concatenate([pair[:, :width], pair[:, width:]], axis=0)


def stacked_rope(rope_pair, rope):
    lane = lax.broadcasted_iota(jnp.int32, rope_pair.shape, 1)
    zero = jnp.zeros_like(rope_pair)
    return jnp.concatenate(
        [jnp.where(lane < rope, rope_pair, zero), jnp.where(lane >= rope, rope_pair, zero)], axis=0
    )


def forward_kernel(dims, info_ref, q_ref, r_ref, u_ref, *refs):
    nd, tokens, shard, latent, rope, scale = dims
    key_refs = refs[:nd]
    ds_ref = refs[nd]
    grad_refs = refs[nd + 1 : 2 * nd + 1]
    keys, s_scr, p_scr, w_scr, acc = refs[2 * nd + 1 :]
    step = pl.program_id(0)

    @pl.when(step == 0)
    def _():
        for d in range(nd):
            keys[d * tokens : (d + 1) * tokens, :] = key_refs[d][...]
        acc[...] = jnp.zeros_like(acc)

    q2 = jnp.concatenate(
        [stacked_pair(q_ref[...], latent), stacked_rope(r_ref[...], rope)], axis=1
    )
    u2 = stacked_pair(u_ref[...], latent)
    nt = (((1,), (1,)), ((), ()))
    s_scr[...] = lax.dot_general(keys[...], q2, nt, preferred_element_type=F32)
    p_scr[...] = lax.dot_general(keys[:, :latent], u2, nt, preferred_element_type=F32)

    row = lax.broadcasted_iota(jnp.int32, (tokens, 2 * tokens), 0)
    col = lax.broadcasted_iota(jnp.int32, (tokens, 2 * tokens), 1)
    slots = tokens // shard
    owner = lax.rem(info_ref[nd] - row // shard + slots, slots)
    key_token = owner * shard + lax.rem(row, shard)
    causal = key_token <= lax.rem(col, tokens)
    peak = None
    for d in range(nd):
        rows = slice(d * tokens, (d + 1) * tokens)
        allowed = info_ref[d] >= 0
        if d == 0:
            allowed = jnp.logical_and(causal, allowed)
        s = jnp.where(allowed, s_scr[rows, :] * (scale * LOG2E), -jnp.inf)
        s_scr[rows, :] = s
        top = jnp.max(s, axis=0, keepdims=True)
        peak = top if peak is None else jnp.maximum(peak, top)
    total = jnp.zeros_like(peak)
    mixed = jnp.zeros_like(peak)
    for d in range(nd):
        rows = slice(d * tokens, (d + 1) * tokens)
        e = jnp.exp2(s_scr[rows, :] - peak)
        s_scr[rows, :] = e
        total += jnp.sum(e, axis=0, keepdims=True)
        mixed += jnp.sum(e * p_scr[rows, :], axis=0, keepdims=True)
    inverse = 1.0 / total
    correction = mixed * inverse
    scaled = inverse * scale
    for d in range(nd):
        rows = slice(d * tokens, (d + 1) * tokens)
        e = s_scr[rows, :]
        w_scr[rows, :] = (e * inverse).astype(BF16)
        ds_ref[rows, :] = (e * scaled * (p_scr[rows, :] - correction)).astype(BF16)
    nn = (((1,), (0,)), ((), ()))
    acc[...] += lax.dot_general(ds_ref[...], q2, nn, preferred_element_type=F32)
    acc[:, :latent] += lax.dot_general(w_scr[...], u2, nn, preferred_element_type=F32)

    @pl.when(step == pl.num_programs(0) - 1)
    def _():
        for d in range(nd):
            grad_refs[d][...] = acc[d * tokens : (d + 1) * tokens, :].astype(grad_refs[d].dtype)


def query_kernel(dims, ds_ref, *refs):
    nd, tokens, latent, rope = dims
    key_refs = refs[:nd]
    dq_ref, dr_ref, keys = refs[nd:]

    @pl.when(pl.program_id(0) == 0)
    def _():
        for d in range(nd):
            keys[d * tokens : (d + 1) * tokens, :] = key_refs[d][...]

    tn = (((0,), (0,)), ((), ()))
    dq = lax.dot_general(ds_ref[...], keys[...], tn, preferred_element_type=F32)
    even, odd = dq[:tokens], dq[tokens:]
    dq_ref[:, :latent] = even[:, :latent].astype(BF16)
    dq_ref[:, latent:] = odd[:, :latent].astype(BF16)
    lane = lax.broadcasted_iota(jnp.int32, (tokens, 2 * rope), 1)
    dr_ref[...] = jnp.where(lane < rope, even[:, latent:], odd[:, latent:]).astype(BF16)


def per_device(query_latent, query_rotary, upstream, latent, key_rotary, pattern):
    spacing = spacing_list(lax.axis_size("blk"))
    nd = len(spacing)
    inner = lax.axis_size("inner")
    tokens = query_latent.shape[0]
    shard, width = latent.shape
    rope = key_rotary.shape[1]
    heads = query_latent.shape[1] // width
    pairs = heads // 2
    wide = width + 2 * rope
    depth = nd * tokens
    scale = (NOPE + rope) ** (-0.5)

    own = jnp.concatenate([latent, key_rotary, key_rotary], axis=1)
    near = jnp.concatenate([own] + [rotated(own, "inner", k) for k in range(1, inner)], axis=0)
    keys = [near] + [rotated(near, "blk", d) for d in spacing[1:]]
    info = jnp.concatenate([pattern[0, :nd], lax.axis_index("inner").astype(jnp.int32)[None]])

    whole = lambda shape: pl.BlockSpec(shape, lambda p: (0, 0))
    column = lambda rows, cols: pl.BlockSpec((rows, cols), lambda p: (0, p))
    key_specs = [whole((tokens, wide))] * nd
    rows = heads * tokens
    ds, *grads = pl.pallas_call(
        functools.partial(forward_kernel, (nd, tokens, shard, width, rope, scale)),
        grid=(pairs,),
        in_specs=[
            pl.BlockSpec(memory_space=pltpu.SMEM),
            column(tokens, 2 * width),
            column(tokens, 2 * rope),
            column(tokens, 2 * width),
        ]
        + key_specs,
        out_specs=[column(depth, 2 * tokens)] + key_specs,
        out_shape=[jax.ShapeDtypeStruct((depth, rows), BF16)]
        + [jax.ShapeDtypeStruct((tokens, wide), F32 if d == 0 else BF16) for d in spacing],
        scratch_shapes=[
            pltpu.VMEM((depth, wide), BF16),
            pltpu.VMEM((depth, 2 * tokens), F32),
            pltpu.VMEM((depth, 2 * tokens), F32),
            pltpu.VMEM((depth, 2 * tokens), BF16),
            pltpu.VMEM((depth, wide), F32),
        ],
        cost_estimate=pl.CostEstimate(
            flops=2 * rows * depth * (2 * wide + 2 * width),
            bytes_accessed=2 * rows * (2 * wide + depth),
            transcendentals=rows * depth,
        ),
        name="scores_and_keys",
    )(info, query_latent, query_rotary, upstream, *keys)

    back = [rotated(g, "blk", -d) for g, d in zip(grads[1:], spacing[1:])]

    query_cotangent, rotary_cotangent = pl.pallas_call(
        functools.partial(query_kernel, (nd, tokens, width, rope)),
        grid=(pairs,),
        in_specs=[column(depth, 2 * tokens)] + key_specs,
        out_specs=[column(tokens, 2 * width), column(tokens, 2 * rope)],
        out_shape=[
            jax.ShapeDtypeStruct(query_latent.shape, BF16),
            jax.ShapeDtypeStruct(query_rotary.shape, BF16),
        ],
        scratch_shapes=[pltpu.VMEM((depth, wide), BF16)],
        cost_estimate=pl.CostEstimate(
            flops=2 * rows * depth * wide,
            bytes_accessed=2 * rows * (wide + depth),
            transcendentals=0,
        ),
        name="query_cotangents",
    )(ds, *keys)

    total = grads[0] + sum(b.astype(F32) for b in back)
    parts = [total[k * shard : (k + 1) * shard] for k in range(inner)]
    final = parts[0] + sum(
        rotated(parts[k].astype(BF16), "inner", -k).astype(F32) for k in range(1, inner)
    )
    latent_cotangent = final[:, :width]
    positional_cotangent = final[:, width : width + rope] + final[:, width + rope :]
    return (query_cotangent, rotary_cotangent, latent_cotangent, positional_cotangent)


def solution(mesh):
    in_specs = (
        P("blk", "inner"),
        P("blk", "inner"),
        P("blk", "inner"),
        P(("blk", "inner"), None),
        P(("blk", "inner"), None),
        P("blk", None),
    )
    out_specs = (
        P("blk", "inner"),
        P("blk", "inner"),
        P(("blk", "inner"), None),
        P(("blk", "inner"), None),
    )
    return jax.shard_map(
        per_device, mesh=mesh, in_specs=in_specs, out_specs=out_specs, check_vma=False
    )
```

```python
import functools

import jax
import jax.numpy as jnp
from jax import lax
from jax.experimental import pallas as pl
from jax.experimental.pallas import tpu as pltpu
from jax.sharding import PartitionSpec as P

NOPE = 128
WIN = 2
NSTR = 4
LOG2E = 1.4426950408889634
BF16 = jnp.bfloat16
F32 = jnp.float32


def spacing_list(blocks):
    spacing = blocks // 8
    listed = set(range(WIN))
    for number in range(1, NSTR + 1):
        listed.add(number * spacing)
    return sorted(listed)


def rotated(value, axis, steps):
    count = lax.axis_size(axis)
    return lax.ppermute(value, axis, [(s, (s + steps) % count) for s in range(count)])


def swapped(value):
    count = lax.axis_size("blk")
    return lax.ppermute(value, "blk", [(s, s + 1 - 2 * (s % 2)) for s in range(count)])


def stacked_pair(pair, width):
    return jnp.concatenate([pair[:, :width], pair[:, width:]], axis=0)


def stacked_rope(rope_pair, rope):
    lane = lax.broadcasted_iota(jnp.int32, rope_pair.shape, 1)
    zero = jnp.zeros_like(rope_pair)
    return jnp.concatenate(
        [jnp.where(lane < rope, rope_pair, zero), jnp.where(lane >= rope, rope_pair, zero)], axis=0
    )


def gradient_pair(ds, weights, q2, u2, grad_ref, latent):
    nn = (((1,), (0,)), ((), ()))
    part = lax.dot_general(ds, q2, nn, preferred_element_type=F32)
    mixed = lax.dot_general(weights, u2, nn, preferred_element_type=F32)
    grad_ref[:, :latent] += part[:, :latent] + mixed
    grad_ref[:, latent:] += part[:, latent:]


def query_pair(ds, keys, dq_ref, dr_ref, tokens, latent, rope):
    tn = (((0,), (0,)), ((), ()))
    dq = lax.dot_general(ds, keys, tn, preferred_element_type=F32)
    even, odd = dq[:tokens], dq[tokens:]
    dq_ref[:, :latent] = even[:, :latent].astype(BF16)
    dq_ref[:, latent:] = odd[:, :latent].astype(BF16)
    lane = lax.broadcasted_iota(jnp.int32, (tokens, 2 * rope), 1)
    dr_ref[...] = jnp.where(lane < rope, even[:, latent:], odd[:, latent:]).astype(BF16)


def scores_kernel(dims, sources, info_ref, q_ref, r_ref, u_ref, *refs):
    nd, kept, tokens, shard, latent, rope, scale = dims
    sent = nd - kept
    ds_ref, kept_ref, keys, grad_ref, s_scr, p_scr, w_scr, acc = refs[-8:]
    key_refs = refs[:-8]
    step = pl.program_id(0)

    @pl.when(step == 0)
    def _():
        for d, source in enumerate(sources):
            rows = slice(d * tokens, (d + 1) * tokens)
            if len(source) == 1:
                keys[rows, :] = key_refs[source[0]][...]
            else:
                odd = info_ref[nd + 1] == 1

                @pl.when(odd)
                def _(rows=rows, source=source):
                    keys[rows, :] = key_refs[source[1]][...]

                @pl.when(jnp.logical_not(odd))
                def _(rows=rows, source=source):
                    keys[rows, :] = key_refs[source[0]][...]

        acc[...] = jnp.zeros_like(acc)

    q2 = jnp.concatenate(
        [stacked_pair(q_ref[...], latent), stacked_rope(r_ref[...], rope)], axis=1
    )
    u2 = stacked_pair(u_ref[...], latent)
    nt = (((1,), (1,)), ((), ()))
    s_scr[...] = lax.dot_general(keys[...], q2, nt, preferred_element_type=F32)
    p_scr[...] = lax.dot_general(keys[:, :latent], u2, nt, preferred_element_type=F32)

    row = lax.broadcasted_iota(jnp.int32, (tokens, 2 * tokens), 0)
    col = lax.broadcasted_iota(jnp.int32, (tokens, 2 * tokens), 1)
    slots = tokens // shard
    owner = lax.rem(info_ref[nd] - row // shard + slots, slots)
    key_token = owner * shard + lax.rem(row, shard)
    causal = key_token <= lax.rem(col, tokens)
    peak = None
    for d in range(nd):
        rows = slice(d * tokens, (d + 1) * tokens)
        allowed = info_ref[d] >= 0
        if d == kept - 1:
            allowed = jnp.logical_and(causal, allowed)
        s = jnp.where(allowed, s_scr[rows, :] * (scale * LOG2E), -jnp.inf)
        s_scr[rows, :] = s
        top = jnp.max(s, axis=0, keepdims=True)
        peak = top if peak is None else jnp.maximum(peak, top)
    total = jnp.zeros_like(peak)
    mixed = jnp.zeros_like(peak)
    for d in range(nd):
        rows = slice(d * tokens, (d + 1) * tokens)
        e = jnp.exp2(s_scr[rows, :] - peak)
        s_scr[rows, :] = e
        total += jnp.sum(e, axis=0, keepdims=True)
        mixed += jnp.sum(e * p_scr[rows, :], axis=0, keepdims=True)
    inverse = 1.0 / total
    correction = mixed * inverse
    scaled = inverse * scale
    for d in range(nd):
        rows = slice(d * tokens, (d + 1) * tokens)
        e = s_scr[rows, :]
        w = (e * inverse).astype(BF16)
        if d < kept:
            kept_ref[rows, :] = w
        else:
            w_scr[(d - kept) * tokens : (d - kept + 1) * tokens, :] = w
        ds_ref[rows, :] = (e * scaled * (p_scr[rows, :] - correction)).astype(BF16)
    gradient_pair(ds_ref[kept * tokens :, :], w_scr[...], q2, u2, acc, latent)

    @pl.when(step == pl.num_programs(0) - 1)
    def _():
        grad_ref[...] = acc[...].astype(BF16)


def gradient_kernel(dims, ds_ref, w_ref, q_ref, r_ref, u_ref, grad_ref):
    latent, rope = dims

    @pl.when(pl.program_id(0) == 0)
    def _():
        grad_ref[...] = jnp.zeros_like(grad_ref)

    q2 = jnp.concatenate(
        [stacked_pair(q_ref[...], latent), stacked_rope(r_ref[...], rope)], axis=1
    )
    gradient_pair(ds_ref[...], w_ref[...], q2, stacked_pair(u_ref[...], latent), grad_ref, latent)


def own_kernel(dims, ds_ref, w_ref, q_ref, r_ref, u_ref, keys_ref, grad_ref, dq_ref, dr_ref):
    own, first, tokens, latent, rope = dims
    step = pl.program_id(0)

    @pl.when(step == 0)
    def _():
        grad_ref[...] = jnp.zeros_like(grad_ref)

    q2 = jnp.concatenate(
        [stacked_pair(q_ref[...], latent), stacked_rope(r_ref[...], rope)], axis=1
    )
    rows = slice(own * tokens, (own + 1) * tokens)
    gradient_pair(ds_ref[rows, :], w_ref[...], q2, stacked_pair(u_ref[...], latent), grad_ref, latent)

    @pl.when(step < first)
    def _():
        query_pair(ds_ref[...], keys_ref[...], dq_ref, dr_ref, tokens, latent, rope)


def rest_kernel(dims, ds_ref, keys_ref, dq_in, dr_in, dq_ref, dr_ref):
    tokens, latent, rope = dims
    query_pair(ds_ref[...], keys_ref[...], dq_ref, dr_ref, tokens, latent, rope)


def per_device(query_latent, query_rotary, upstream, latent, key_rotary, pattern):
    blocks = lax.axis_size("blk")
    spacing = spacing_list(blocks)
    nd = len(spacing)
    inner = lax.axis_size("inner")
    tokens = query_latent.shape[0]
    shard, width = latent.shape
    rope = key_rotary.shape[1]
    heads = query_latent.shape[1] // width
    pairs = heads // 2
    first = pairs // 2
    wide = width + 2 * rope
    depth = nd * tokens
    rows = heads * tokens
    scale = (NOPE + rope) ** (-0.5)
    paired = spacing == [0, 1, 2, 3, 4] and blocks % 2 == 0

    own = jnp.concatenate([latent, key_rotary, key_rotary], axis=1)
    near = jnp.concatenate([own] + [rotated(own, "inner", k) for k in range(1, inner)], axis=0)
    odd = lax.rem(lax.axis_index("blk"), 2).astype(jnp.int32)
    if paired:
        order = [2, 4, 0, 1, 3]
        kept = 3
        two, four = rotated(near, "blk", 2), rotated(near, "blk", 4)
        sources = [(0,), (1,), (2,), (4, 3), (5, 4)]
        key_arrays = [two, four, near, swapped(near), swapped(two), swapped(four)]
    else:
        order = spacing
        kept = 1
        sources = [(d,) for d in range(nd)]
        key_arrays = [near] + [rotated(near, "blk", d) for d in spacing[1:]]
    sent = nd - kept
    picked = [pattern[0, spacing.index(d)] for d in order]
    info = jnp.stack(picked + [lax.axis_index("inner").astype(jnp.int32), odd])

    whole = lambda shape: pl.BlockSpec(shape, lambda p: (0, 0))
    column = lambda height, cols, base=0: pl.BlockSpec((height, cols), lambda p: (base, p))
    query_specs = [column(tokens, 2 * width), column(tokens, 2 * rope), column(tokens, 2 * width)]
    queries = (query_latent, query_rotary, upstream)
    ds, weights, keys, grads = pl.pallas_call(
        functools.partial(
            scores_kernel, (nd, kept, tokens, shard, width, rope, scale), sources
        ),
        grid=(pairs,),
        in_specs=[pl.BlockSpec(memory_space=pltpu.SMEM)]
        + query_specs
        + [whole((tokens, wide))] * len(key_arrays),
        out_specs=[
            column(depth, 2 * tokens),
            column(kept * tokens, 2 * tokens),
            whole((depth, wide)),
            whole((sent * tokens, wide)),
        ],
        out_shape=[
            jax.ShapeDtypeStruct((depth, rows), BF16),
            jax.ShapeDtypeStruct((kept * tokens, rows), BF16),
            jax.ShapeDtypeStruct((depth, wide), BF16),
            jax.ShapeDtypeStruct((sent * tokens, wide), BF16),
        ],
        scratch_shapes=[
            pltpu.VMEM((depth, 2 * tokens), F32),
            pltpu.VMEM((depth, 2 * tokens), F32),
            pltpu.VMEM((sent * tokens, 2 * tokens), BF16),
            pltpu.VMEM((sent * tokens, wide), F32),
        ],
        cost_estimate=pl.CostEstimate(
            flops=2 * rows * (depth + sent * tokens) * (wide + width),
            bytes_accessed=2 * rows * (2 * wide + depth),
            transcendentals=rows * depth,
        ),
        name="scores",
    )(info, *queries, *key_arrays)

    if paired:
        met = swapped(grads)
        late = pl.pallas_call(
            functools.partial(gradient_kernel, (width, rope)),
            grid=(pairs,),
            in_specs=[
                column((kept - 1) * tokens, 2 * tokens),
                column((kept - 1) * tokens, 2 * tokens),
            ]
            + query_specs,
            out_specs=whole(((kept - 1) * tokens, wide)),
            out_shape=jax.ShapeDtypeStruct(((kept - 1) * tokens, wide), F32),
            cost_estimate=pl.CostEstimate(
                flops=2 * rows * (kept - 1) * tokens * (wide + width),
                bytes_accessed=4 * rows * wide,
                transcendentals=0,
            ),
            name="late_gradients",
        )(ds, weights, *queries)
        met_one, met_three = met[:tokens].astype(F32), met[tokens:].astype(F32)
        to_two = late[:tokens] + jnp.where(odd == 1, met_one, met_three)
        to_four = late[tokens:] + jnp.where(odd == 1, met_three, 0.0)
        back = [
            rotated(to_two.astype(BF16), "blk", -2).astype(F32),
            rotated(to_four.astype(BF16), "blk", -4).astype(F32),
            jnp.where(odd == 1, 0.0, met_one),
        ]
    else:
        back = [
            rotated(grads[k * tokens : (k + 1) * tokens], "blk", -d).astype(F32)
            for k, d in enumerate(spacing[1:])
        ]

    own_grad, dq, dr = pl.pallas_call(
        functools.partial(own_kernel, (kept - 1, first, tokens, width, rope)),
        grid=(pairs,),
        in_specs=[column(depth, 2 * tokens), column(tokens, 2 * tokens, kept - 1)]
        + query_specs
        + [whole((depth, wide))],
        out_specs=[
            whole((tokens, wide)),
            pl.BlockSpec((tokens, 2 * width), lambda p: (0, jnp.minimum(p, first - 1))),
            pl.BlockSpec((tokens, 2 * rope), lambda p: (0, jnp.minimum(p, first - 1))),
        ],
        out_shape=[
            jax.ShapeDtypeStruct((tokens, wide), F32),
            jax.ShapeDtypeStruct(query_latent.shape, BF16),
            jax.ShapeDtypeStruct(query_rotary.shape, BF16),
        ],
        cost_estimate=pl.CostEstimate(
            flops=2 * rows * tokens * (wide + width) + rows * depth * wide,
            bytes_accessed=2 * rows * (wide + depth),
            transcendentals=0,
        ),
        name="own_gradients",
    )(ds, weights, *queries, keys)

    total = own_grad + sum(back)
    parts = [total[k * shard : (k + 1) * shard] for k in range(inner)]
    moved = [rotated(parts[k].astype(BF16), "inner", -k).astype(F32) for k in range(1, inner)]

    later = lambda height, cols: pl.BlockSpec((height, cols), lambda p: (0, p + first))
    query_cotangent, rotary_cotangent = pl.pallas_call(
        functools.partial(rest_kernel, (tokens, width, rope)),
        grid=(pairs - first,),
        in_specs=[
            later(depth, 2 * tokens),
            whole((depth, wide)),
            pl.BlockSpec(memory_space=pl.ANY),
            pl.BlockSpec(memory_space=pl.ANY),
        ],
        out_specs=[later(tokens, 2 * width), later(tokens, 2 * rope)],
        out_shape=[
            jax.ShapeDtypeStruct(query_latent.shape, BF16),
            jax.ShapeDtypeStruct(query_rotary.shape, BF16),
        ],
        input_output_aliases={2: 0, 3: 1},
        cost_estimate=pl.CostEstimate(
            flops=rows * depth * wide,
            bytes_accessed=rows * (wide + depth),
            transcendentals=0,
        ),
        name="query_cotangents",
    )(ds, keys, dq, dr)

    final = parts[0] + sum(moved)
    latent_cotangent = final[:, :width]
    positional_cotangent = final[:, width : width + rope] + final[:, width + rope :]
    return (query_cotangent, rotary_cotangent, latent_cotangent, positional_cotangent)


def solution(mesh):
    in_specs = (
        P("blk", "inner"),
        P("blk", "inner"),
        P("blk", "inner"),
        P(("blk", "inner"), None),
        P(("blk", "inner"), None),
        P("blk", None),
    )
    out_specs = (
        P("blk", "inner"),
        P("blk", "inner"),
        P(("blk", "inner"), None),
        P(("blk", "inner"), None),
    )
    return jax.shard_map(
        per_device, mesh=mesh, in_specs=in_specs, out_specs=out_specs, check_vma=False
    )
```

```python
import functools

import jax
import jax.numpy as jnp
from jax import lax
from jax.experimental import pallas as pl
from jax.experimental.pallas import tpu as pltpu
from jax.sharding import PartitionSpec as P

NOPE = 128
WIN = 2
NSTR = 4
LOG2E = 1.4426950408889634
BF16 = jnp.bfloat16
F32 = jnp.float32
VMEM = 24 * 1024 * 1024


def spacing_list(blocks):
    spacing = blocks // 8
    listed = set(range(WIN))
    for number in range(1, NSTR + 1):
        listed.add(number * spacing)
    return sorted(listed)


def rotated(value, axis, steps):
    count = lax.axis_size(axis)
    return lax.ppermute(value, axis, [(s, (s + steps) % count) for s in range(count)])


def swapped(value):
    count = lax.axis_size("blk")
    return lax.ppermute(value, "blk", [(s, s + 1 - 2 * (s % 2)) for s in range(count)])


def stacked_pair(pair, width):
    return jnp.concatenate([pair[:, :width], pair[:, width:]], axis=0)


def stacked_rope(rope_pair, rope):
    lane = lax.broadcasted_iota(jnp.int32, rope_pair.shape, 1)
    zero = jnp.zeros_like(rope_pair)
    return jnp.concatenate(
        [jnp.where(lane < rope, rope_pair, zero), jnp.where(lane >= rope, rope_pair, zero)], axis=0
    )


def stage_kernel(dims, q_ref, r_ref, u_ref, q2_ref, u2_ref, rope_scr, sems):
    heads, tokens, latent, rope = dims
    copies = [pltpu.make_async_copy(r_ref, rope_scr, sems.at[2 * heads])]
    for h in range(heads):
        rows = slice(h * tokens, (h + 1) * tokens)
        cols = slice(h * latent, (h + 1) * latent)
        copies.append(
            pltpu.make_async_copy(q_ref.at[:, cols], q2_ref.at[rows, :latent], sems.at[h])
        )
        copies.append(
            pltpu.make_async_copy(u_ref.at[:, cols], u2_ref.at[rows, :], sems.at[heads + h])
        )
    for copy in copies:
        copy.start()
    copies[0].wait()
    for p in range(heads // 2):
        rows = slice(2 * p * tokens, 2 * (p + 1) * tokens)
        q2_ref[rows, latent:] = stacked_rope(rope_scr[:, 2 * p * rope : 2 * (p + 1) * rope], rope)
    for copy in copies[1:]:
        copy.wait()


def merge_kernel(late_ref, met_ref, two_ref, four_ref):
    tokens = two_ref.shape[0]
    odd = lax.rem(lax.axis_index("blk"), 2) == 1
    one, three = met_ref[:tokens].astype(F32), met_ref[tokens:].astype(F32)
    two_ref[...] = (late_ref[:tokens] + jnp.where(odd, one, three)).astype(BF16)
    four_ref[...] = (late_ref[tokens:] + jnp.where(odd, three, 0.0)).astype(BF16)


def total_kernel(returned, own_ref, *refs):
    total = own_ref[...]
    for ref in refs[:returned]:
        total += ref[...].astype(F32)
    for k, ref in enumerate(refs[returned:]):
        shard = ref.shape[0]
        ref[...] = total[k * shard : (k + 1) * shard].astype(ref.dtype)


def finish_kernel(dims, own_ref, *refs):
    latent, rope = dims
    *parts, latent_ref, rope_ref = refs
    total = own_ref[...]
    for part in parts:
        total += part[...].astype(F32)
    latent_ref[...] = total[:, :latent]
    rope_ref[...] = total[:, latent : latent + rope] + total[:, latent + rope :]


def gradient_pair(ds, weights, q2, u2, grad_ref, latent):
    nn = (((1,), (0,)), ((), ()))
    part = lax.dot_general(ds, q2, nn, preferred_element_type=F32)
    mixed = lax.dot_general(weights, u2, nn, preferred_element_type=F32)
    grad_ref[:, :latent] += part[:, :latent] + mixed
    grad_ref[:, latent:] += part[:, latent:]


def query_pair(ds, keys, dq_ref, dr_ref, tokens, latent, rope):
    tn = (((0,), (0,)), ((), ()))
    dq = lax.dot_general(ds, keys, tn, preferred_element_type=F32)
    even, odd = dq[:tokens], dq[tokens:]
    dq_ref[:, :latent] = even[:, :latent].astype(BF16)
    dq_ref[:, latent:] = odd[:, :latent].astype(BF16)
    lane = lax.broadcasted_iota(jnp.int32, (tokens, 2 * rope), 1)
    dr_ref[...] = jnp.where(lane < rope, even[:, latent:], odd[:, latent:]).astype(BF16)


def scores_kernel(dims, sources, entries, pattern_ref, q2_ref, u2_ref, *refs):
    nd, kept, tokens, shard, latent, rope, scale = dims
    sent = nd - kept
    ds_ref, kept_ref, keys, grad_ref, s_scr, p_scr, w_scr, acc = refs[-8:]
    key_refs = refs[:-8]
    step = pl.program_id(0)

    @pl.when(step == 0)
    def _():
        for d, source in enumerate(sources):
            rows = slice(d * tokens, (d + 1) * tokens)
            if len(source) == 1:
                keys[rows, :] = key_refs[source[0]][...]
            else:
                odd = lax.rem(lax.axis_index("blk"), 2) == 1

                @pl.when(odd)
                def _(rows=rows, source=source):
                    keys[rows, :] = key_refs[source[1]][...]

                @pl.when(jnp.logical_not(odd))
                def _(rows=rows, source=source):
                    keys[rows, :] = key_refs[source[0]][...]

        acc[...] = jnp.zeros_like(acc)

    q2 = q2_ref[...]
    u2 = u2_ref[...]
    nt = (((1,), (1,)), ((), ()))
    s_scr[...] = lax.dot_general(keys[...], q2, nt, preferred_element_type=F32)
    p_scr[...] = lax.dot_general(keys[:, :latent], u2, nt, preferred_element_type=F32)

    row = lax.broadcasted_iota(jnp.int32, (tokens, 2 * tokens), 0)
    col = lax.broadcasted_iota(jnp.int32, (tokens, 2 * tokens), 1)
    slots = tokens // shard
    owner = lax.rem(lax.axis_index("inner") - row // shard + slots, slots)
    key_token = owner * shard + lax.rem(row, shard)
    causal = key_token <= lax.rem(col, tokens)
    peak = None
    for d in range(nd):
        rows = slice(d * tokens, (d + 1) * tokens)
        allowed = pattern_ref[0, entries[d]] >= 0
        if d == kept - 1:
            allowed = jnp.logical_and(causal, allowed)
        s = jnp.where(allowed, s_scr[rows, :] * (scale * LOG2E), -jnp.inf)
        s_scr[rows, :] = s
        top = jnp.max(s, axis=0, keepdims=True)
        peak = top if peak is None else jnp.maximum(peak, top)
    total = jnp.zeros_like(peak)
    mixed = jnp.zeros_like(peak)
    for d in range(nd):
        rows = slice(d * tokens, (d + 1) * tokens)
        e = jnp.exp2(s_scr[rows, :] - peak)
        s_scr[rows, :] = e
        total += jnp.sum(e, axis=0, keepdims=True)
        mixed += jnp.sum(e * p_scr[rows, :], axis=0, keepdims=True)
    inverse = 1.0 / total
    correction = mixed * inverse
    scaled = inverse * scale
    for d in range(nd):
        rows = slice(d * tokens, (d + 1) * tokens)
        e = s_scr[rows, :]
        w = (e * inverse).astype(BF16)
        if d < kept:
            kept_ref[rows, :] = w
        else:
            w_scr[(d - kept) * tokens : (d - kept + 1) * tokens, :] = w
        ds_ref[rows, :] = (e * scaled * (p_scr[rows, :] - correction)).astype(BF16)
    gradient_pair(ds_ref[kept * tokens :, :], w_scr[...], q2, u2, acc, latent)

    @pl.when(step == pl.num_programs(0) - 1)
    def _():
        grad_ref[...] = acc[...].astype(BF16)


def gradient_kernel(dims, ds_ref, w_ref, q2_ref, u2_ref, grad_ref):
    (latent,) = dims

    @pl.when(pl.program_id(0) == 0)
    def _():
        grad_ref[...] = jnp.zeros_like(grad_ref)

    gradient_pair(ds_ref[...], w_ref[...], q2_ref[...], u2_ref[...], grad_ref, latent)


def own_kernel(dims, ds_ref, w_ref, q2_ref, u2_ref, keys_ref, *refs):
    own, first, tokens, latent, rope = dims
    *met_refs, grad_ref, dq_ref, dr_ref = refs
    step = pl.program_id(0)

    @pl.when(step == 0)
    def _():
        start = jnp.zeros_like(grad_ref)
        for ref in met_refs:
            odd = lax.rem(lax.axis_index("blk"), 2) == 1
            start = jnp.where(odd, start, ref[...].astype(F32))
        grad_ref[...] = start

    rows = slice(own * tokens, (own + 1) * tokens)
    gradient_pair(ds_ref[rows, :], w_ref[...], q2_ref[...], u2_ref[...], grad_ref, latent)

    @pl.when(step < first)
    def _():
        query_pair(ds_ref[...], keys_ref[...], dq_ref, dr_ref, tokens, latent, rope)


def rest_kernel(dims, ds_ref, keys_ref, dq_in, dr_in, dq_ref, dr_ref):
    tokens, latent, rope = dims
    query_pair(ds_ref[...], keys_ref[...], dq_ref, dr_ref, tokens, latent, rope)


def per_device(query_latent, query_rotary, upstream, latent, key_rotary, pattern):
    blocks = lax.axis_size("blk")
    spacing = spacing_list(blocks)
    nd = len(spacing)
    inner = lax.axis_size("inner")
    tokens = query_latent.shape[0]
    shard, width = latent.shape
    rope = key_rotary.shape[1]
    heads = query_latent.shape[1] // width
    pairs = heads // 2
    first = pairs // 2
    wide = width + 2 * rope
    depth = nd * tokens
    rows = heads * tokens
    scale = (NOPE + rope) ** (-0.5)
    paired = spacing == [0, 1, 2, 3, 4] and blocks % 2 == 0

    whole = lambda shape: pl.BlockSpec(shape, lambda p: (0, 0))
    column = lambda height, cols, base=0: pl.BlockSpec((height, cols), lambda p: (base, p))
    block = lambda height, cols: pl.BlockSpec((height, cols), lambda p: (p, 0))
    query_specs = [block(2 * tokens, wide), block(2 * tokens, width)]
    hbm = pl.BlockSpec(memory_space=pltpu.HBM)
    vmem = pl.BlockSpec(memory_space=pltpu.VMEM)
    queries = pl.pallas_call(
        functools.partial(stage_kernel, (heads, tokens, width, rope)),
        in_specs=[hbm] * 3,
        out_specs=[vmem] * 2,
        out_shape=[
            jax.ShapeDtypeStruct((rows, wide), BF16),
            jax.ShapeDtypeStruct((rows, width), BF16),
        ],
        scratch_shapes=[
            pltpu.VMEM((tokens, heads * rope), BF16),
            pltpu.SemaphoreType.DMA((2 * heads + 1,)),
        ],
        cost_estimate=pl.CostEstimate(
            flops=2 * rows * wide * width, bytes_accessed=8 * rows * wide, transcendentals=0
        ),
        compiler_params=pltpu.CompilerParams(vmem_limit_bytes=VMEM),
        name="stage",
    )(query_latent, query_rotary, upstream)

    own = jnp.concatenate([latent, key_rotary, key_rotary], axis=1)
    gathered = [own] + [rotated(own, "inner", k) for k in range(1, inner)]
    gathered, queries = lax.optimization_barrier((gathered, queries))
    near = jnp.concatenate(gathered, axis=0)
    if paired:
        order = [2, 4, 0, 1, 3]
        kept = 3
        two, four = rotated(near, "blk", 2), rotated(near, "blk", 4)
        sources = [(0,), (1,), (2,), (4, 3), (5, 4)]
        key_arrays = [two, four, near, swapped(near), swapped(two), swapped(four)]
    else:
        order = spacing
        kept = 1
        sources = [(d,) for d in range(nd)]
        key_arrays = [near] + [rotated(near, "blk", d) for d in spacing[1:]]
    sent = nd - kept
    entries = [spacing.index(d) for d in order]

    ds, weights, keys, grads = pl.pallas_call(
        functools.partial(
            scores_kernel, (nd, kept, tokens, shard, width, rope, scale), sources, entries
        ),
        grid=(pairs,),
        in_specs=[pl.BlockSpec(memory_space=pltpu.SMEM)]
        + query_specs
        + [whole((tokens, wide))] * len(key_arrays),
        out_specs=[
            column(depth, 2 * tokens),
            column(kept * tokens, 2 * tokens),
            whole((depth, wide)),
            whole((sent * tokens, wide)),
        ],
        out_shape=[
            jax.ShapeDtypeStruct((depth, rows), BF16),
            jax.ShapeDtypeStruct((kept * tokens, rows), BF16),
            jax.ShapeDtypeStruct((depth, wide), BF16),
            jax.ShapeDtypeStruct((sent * tokens, wide), BF16),
        ],
        scratch_shapes=[
            pltpu.VMEM((depth, 2 * tokens), F32),
            pltpu.VMEM((depth, 2 * tokens), F32),
            pltpu.VMEM((sent * tokens, 2 * tokens), BF16),
            pltpu.VMEM((sent * tokens, wide), F32),
        ],
        cost_estimate=pl.CostEstimate(
            flops=2 * rows * (depth + sent * tokens) * (wide + width),
            bytes_accessed=2 * rows * (2 * wide + depth),
            transcendentals=rows * depth,
        ),
        compiler_params=pltpu.CompilerParams(vmem_limit_bytes=VMEM),
        name="scores",
    )(pattern, *queries, *key_arrays)

    if paired:
        met = swapped(grads)
        late = pl.pallas_call(
            functools.partial(gradient_kernel, (width,)),
            grid=(pairs,),
            in_specs=[
                column((kept - 1) * tokens, 2 * tokens),
                column((kept - 1) * tokens, 2 * tokens),
            ]
            + query_specs,
            out_specs=whole(((kept - 1) * tokens, wide)),
            out_shape=jax.ShapeDtypeStruct(((kept - 1) * tokens, wide), F32),
            cost_estimate=pl.CostEstimate(
                flops=2 * rows * (kept - 1) * tokens * (wide + width),
                bytes_accessed=4 * rows * wide,
                transcendentals=0,
            ),
            compiler_params=pltpu.CompilerParams(vmem_limit_bytes=VMEM),
            name="late_gradients",
        )(ds, weights, *queries)
        to_two, to_four = pl.pallas_call(
            merge_kernel,
            out_shape=[jax.ShapeDtypeStruct((tokens, wide), BF16)] * 2,
            compiler_params=pltpu.CompilerParams(vmem_limit_bytes=VMEM),
            name="merge",
        )(late, met)
        back = [rotated(to_two, "blk", -2), rotated(to_four, "blk", -4)]
        handed = [met]
    else:
        back = [
            rotated(grads[k * tokens : (k + 1) * tokens], "blk", -d)
            for k, d in enumerate(spacing[1:])
        ]
        handed = []

    own_grad, dq, dr = pl.pallas_call(
        functools.partial(own_kernel, (kept - 1, first, tokens, width, rope)),
        grid=(pairs,),
        in_specs=[column(depth, 2 * tokens), column(tokens, 2 * tokens, kept - 1)]
        + query_specs
        + [whole((depth, wide))]
        + [whole((tokens, wide))] * len(handed),
        out_specs=[
            whole((tokens, wide)),
            pl.BlockSpec((tokens, 2 * width), lambda p: (0, jnp.minimum(p, first - 1))),
            pl.BlockSpec((tokens, 2 * rope), lambda p: (0, jnp.minimum(p, first - 1))),
        ],
        out_shape=[
            jax.ShapeDtypeStruct((tokens, wide), F32),
            jax.ShapeDtypeStruct(query_latent.shape, BF16),
            jax.ShapeDtypeStruct(query_rotary.shape, BF16),
        ],
        cost_estimate=pl.CostEstimate(
            flops=2 * rows * tokens * (wide + width) + rows * depth * wide,
            bytes_accessed=2 * rows * (wide + depth),
            transcendentals=0,
        ),
        compiler_params=pltpu.CompilerParams(vmem_limit_bytes=VMEM),
        name="own_gradients",
    )(ds, weights, *queries, keys, *handed)

    parts = pl.pallas_call(
        functools.partial(total_kernel, len(back)),
        out_shape=[
            jax.ShapeDtypeStruct((shard, wide), F32 if k == 0 else BF16) for k in range(inner)
        ],
        compiler_params=pltpu.CompilerParams(vmem_limit_bytes=VMEM),
        name="total",
    )(own_grad, *back)
    moved = [rotated(parts[k], "inner", -k) for k in range(1, inner)]

    later = lambda height, cols: pl.BlockSpec((height, cols), lambda p: (0, p + first))
    query_cotangent, rotary_cotangent = pl.pallas_call(
        functools.partial(rest_kernel, (tokens, width, rope)),
        grid=(pairs - first,),
        in_specs=[
            later(depth, 2 * tokens),
            whole((depth, wide)),
            pl.BlockSpec(memory_space=pl.ANY),
            pl.BlockSpec(memory_space=pl.ANY),
        ],
        out_specs=[later(tokens, 2 * width), later(tokens, 2 * rope)],
        out_shape=[
            jax.ShapeDtypeStruct(query_latent.shape, BF16),
            jax.ShapeDtypeStruct(query_rotary.shape, BF16),
        ],
        input_output_aliases={2: 0, 3: 1},
        cost_estimate=pl.CostEstimate(
            flops=rows * depth * wide,
            bytes_accessed=rows * (wide + depth),
            transcendentals=0,
        ),
        compiler_params=pltpu.CompilerParams(vmem_limit_bytes=VMEM),
        name="query_cotangents",
    )(ds, keys, dq, dr)

    latent_cotangent, positional_cotangent = pl.pallas_call(
        functools.partial(finish_kernel, (width, rope)),
        out_shape=[
            jax.ShapeDtypeStruct((shard, width), F32),
            jax.ShapeDtypeStruct((shard, rope), F32),
        ],
        compiler_params=pltpu.CompilerParams(vmem_limit_bytes=VMEM),
        name="finish",
    )(parts[0], *moved)
    return (query_cotangent, rotary_cotangent, latent_cotangent, positional_cotangent)


def solution(mesh):
    in_specs = (
        P("blk", "inner"),
        P("blk", "inner"),
        P("blk", "inner"),
        P(("blk", "inner"), None),
        P(("blk", "inner"), None),
        P("blk", None),
    )
    out_specs = (
        P("blk", "inner"),
        P("blk", "inner"),
        P(("blk", "inner"), None),
        P(("blk", "inner"), None),
    )
    return jax.shard_map(
        per_device, mesh=mesh, in_specs=in_specs, out_specs=out_specs, check_vma=False
    )
```

```python
import functools

import jax
import jax.numpy as jnp
from jax import lax
from jax.experimental import pallas as pl
from jax.experimental.pallas import tpu as pltpu
from jax.sharding import PartitionSpec as P

NOPE = 128
WIN = 2
NSTR = 4
LOG2E = 1.4426950408889634
BF16 = jnp.bfloat16
F32 = jnp.float32
VMEM = 24 * 1024 * 1024


def spacing_list(blocks):
    spacing = blocks // 8
    listed = set(range(WIN))
    for number in range(1, NSTR + 1):
        listed.add(number * spacing)
    return sorted(listed)


def rotated(value, axis, steps):
    count = lax.axis_size(axis)
    return lax.ppermute(value, axis, [(s, (s + steps) % count) for s in range(count)])


def swapped(value):
    count = lax.axis_size("blk")
    return lax.ppermute(value, "blk", [(s, s + 1 - 2 * (s % 2)) for s in range(count)])


def stacked_pair(pair, width):
    return jnp.concatenate([pair[:, :width], pair[:, width:]], axis=0)


def stacked_rope(rope_pair, rope):
    lane = lax.broadcasted_iota(jnp.int32, rope_pair.shape, 1)
    zero = jnp.zeros_like(rope_pair)
    return jnp.concatenate(
        [jnp.where(lane < rope, rope_pair, zero), jnp.where(lane >= rope, rope_pair, zero)], axis=0
    )


def stage_kernel(dims, q_ref, r_ref, u_ref, q2_ref, u2_ref, rope_scr, sems):
    heads, tokens, latent, rope = dims
    copies = [pltpu.make_async_copy(r_ref, rope_scr, sems.at[2 * heads])]
    for h in range(heads):
        rows = slice(h * tokens, (h + 1) * tokens)
        cols = slice(h * latent, (h + 1) * latent)
        copies.append(
            pltpu.make_async_copy(q_ref.at[:, cols], q2_ref.at[rows, :latent], sems.at[h])
        )
        copies.append(
            pltpu.make_async_copy(u_ref.at[:, cols], u2_ref.at[rows, :], sems.at[heads + h])
        )
    for copy in copies:
        copy.start()
    copies[0].wait()
    for p in range(heads // 2):
        rows = slice(2 * p * tokens, 2 * (p + 1) * tokens)
        q2_ref[rows, latent:] = stacked_rope(rope_scr[:, 2 * p * rope : 2 * (p + 1) * rope], rope)
    for copy in copies[1:]:
        copy.wait()


def merge_kernel(late_ref, met_ref, two_ref, four_ref):
    tokens = two_ref.shape[0]
    odd = lax.rem(lax.axis_index("blk"), 2) == 1
    one, three = met_ref[:tokens].astype(F32), met_ref[tokens:].astype(F32)
    two_ref[...] = (late_ref[:tokens] + jnp.where(odd, one, three)).astype(BF16)
    four_ref[...] = (late_ref[tokens:] + jnp.where(odd, three, 0.0)).astype(BF16)


def total_kernel(returned, own_ref, *refs):
    total = own_ref[...]
    for ref in refs[:returned]:
        total += ref[...].astype(F32)
    for k, ref in enumerate(refs[returned:]):
        shard = ref.shape[0]
        ref[...] = total[k * shard : (k + 1) * shard].astype(ref.dtype)


def finish_kernel(dims, own_ref, *refs):
    latent, rope = dims
    *parts, latent_ref, rope_ref = refs
    total = own_ref[...]
    for part in parts:
        total += part[...].astype(F32)
    latent_ref[...] = total[:, :latent]
    rope_ref[...] = total[:, latent : latent + rope] + total[:, latent + rope :]


def key_gradient(ds, weights, q2, u2, latent):
    nn = (((1,), (0,)), ((), ()))
    part = lax.dot_general(ds, q2, nn, preferred_element_type=F32)
    mixed = lax.dot_general(weights, u2, nn, preferred_element_type=F32)
    return part[:, :latent] + mixed, part[:, latent:]


def scores_kernel(dims, sources, entries, pattern_ref, q2_ref, u2_ref, *refs):
    nd, kept, pairs, tokens, shard, latent, rope, scale = dims
    sent = nd - kept
    ds_ref, kept_ref, keys, grad_ref, s_scr, p_scr, w_scr = refs[-7:]
    key_refs = refs[:-7]
    odd = lax.rem(lax.axis_index("blk"), 2) == 1
    for d, source in enumerate(sources):
        rows = slice(d * tokens, (d + 1) * tokens)
        block = key_refs[source[0]][...]
        if len(source) == 2:
            block = jnp.where(odd, key_refs[source[1]][...], block)
        keys[rows, :] = block

    row = lax.broadcasted_iota(jnp.int32, (tokens, 2 * tokens), 0)
    col = lax.broadcasted_iota(jnp.int32, (tokens, 2 * tokens), 1)
    slots = tokens // shard
    owner = lax.rem(lax.axis_index("inner") - row // shard + slots, slots)
    key_token = owner * shard + lax.rem(row, shard)
    causal = key_token <= lax.rem(col, tokens)
    chosen = [pattern_ref[0, entries[d]] >= 0 for d in range(nd)]
    nt = (((1,), (1,)), ((), ()))
    nn = (((1,), (0,)), ((), ()))

    def products(p):
        lanes = slice(2 * p * tokens, 2 * (p + 1) * tokens)
        s_scr[p % 2] = lax.dot_general(keys[...], q2_ref[lanes, :], nt, preferred_element_type=F32)
        p_scr[p % 2] = lax.dot_general(
            keys[:, :latent], u2_ref[lanes, :], nt, preferred_element_type=F32
        )

    def softmax(p):
        lanes = slice(2 * p * tokens, 2 * (p + 1) * tokens)
        slot = p % 2
        peak = None
        for d in range(nd):
            rows = slice(d * tokens, (d + 1) * tokens)
            allowed = jnp.logical_and(causal, chosen[d]) if d == kept - 1 else chosen[d]
            s = jnp.where(allowed, s_scr[slot, rows, :] * (scale * LOG2E), -jnp.inf)
            s_scr[slot, rows, :] = s
            top = jnp.max(s, axis=0, keepdims=True)
            peak = top if peak is None else jnp.maximum(peak, top)
        total = jnp.zeros_like(peak)
        mixed = jnp.zeros_like(peak)
        for d in range(nd):
            rows = slice(d * tokens, (d + 1) * tokens)
            e = jnp.exp2(s_scr[slot, rows, :] - peak)
            s_scr[slot, rows, :] = e
            total += jnp.sum(e, axis=0, keepdims=True)
            mixed += jnp.sum(e * p_scr[slot, rows, :], axis=0, keepdims=True)
        inverse = 1.0 / total
        correction = mixed * inverse
        scaled = inverse * scale
        for d in range(nd):
            rows = slice(d * tokens, (d + 1) * tokens)
            e = s_scr[slot, rows, :]
            w = (e * inverse).astype(BF16)
            if d < kept:
                kept_ref[rows, lanes] = w
            else:
                w_scr[(d - kept) * tokens : (d - kept + 1) * tokens, lanes] = w
            ds_ref[rows, lanes] = (e * scaled * (p_scr[slot, rows, :] - correction)).astype(BF16)

    products(0)
    for p in range(pairs):
        if p + 1 < pairs:
            products(p + 1)
        softmax(p)
    main, turned = key_gradient(
        ds_ref[kept * tokens :, :], w_scr[...], q2_ref[...], u2_ref[...], latent
    )
    grad_ref[:, :latent] = main.astype(BF16)
    grad_ref[:, latent:] = turned.astype(BF16)


def gradient_kernel(dims, ds_ref, w_ref, q2_ref, u2_ref, grad_ref):
    late, latent = dims
    main, turned = key_gradient(
        ds_ref[:late, :], w_ref[:late, :], q2_ref[...], u2_ref[...], latent
    )
    grad_ref[:, :latent] = main
    grad_ref[:, latent:] = turned


def own_kernel(dims, ds_ref, w_ref, q2_ref, u2_ref, keys_ref, *refs):
    own, pairs, tokens, latent, rope = dims
    *met_refs, grad_ref, dq_ref, dr_ref, dq_scr, dr_scr, sems = refs
    tn = (((0,), (0,)), ((), ()))
    lane = lax.broadcasted_iota(jnp.int32, (tokens, 2 * rope), 1)
    copies = []
    for p in range(pairs):
        lanes = slice(2 * p * tokens, 2 * (p + 1) * tokens)
        dq = lax.dot_general(ds_ref[:, lanes], keys_ref[...], tn, preferred_element_type=F32)
        even, odd = dq[:tokens], dq[tokens:]
        out = 2 * p * latent
        dq_scr[:, out : out + latent] = even[:, :latent].astype(BF16)
        dq_scr[:, out + latent : out + 2 * latent] = odd[:, :latent].astype(BF16)
        turned = jnp.where(lane < rope, even[:, latent:], odd[:, latent:])
        dr_scr[:, 2 * p * rope : 2 * (p + 1) * rope] = turned.astype(BF16)
        cols = slice(out, out + 2 * latent)
        copies.append(pltpu.make_async_copy(dq_scr.at[:, cols], dq_ref.at[:, cols], sems.at[p]))
        copies[-1].start()
    copies.append(pltpu.make_async_copy(dr_scr, dr_ref, sems.at[pairs]))
    copies[-1].start()
    rows = slice(own * tokens, (own + 1) * tokens)
    main, turned = key_gradient(
        ds_ref[rows, :], w_ref[rows, :], q2_ref[...], u2_ref[...], latent
    )
    start = jnp.zeros(grad_ref.shape, F32)
    for ref in met_refs:
        is_odd = lax.rem(lax.axis_index("blk"), 2) == 1
        start = jnp.where(is_odd, start, ref[:tokens, :].astype(F32))
    grad_ref[:, :latent] = start[:, :latent] + main
    grad_ref[:, latent:] = start[:, latent:] + turned
    for copy in copies:
        copy.wait()


def per_device(query_latent, query_rotary, upstream, latent, key_rotary, pattern):
    blocks = lax.axis_size("blk")
    spacing = spacing_list(blocks)
    nd = len(spacing)
    inner = lax.axis_size("inner")
    tokens = query_latent.shape[0]
    shard, width = latent.shape
    rope = key_rotary.shape[1]
    heads = query_latent.shape[1] // width
    pairs = heads // 2
    wide = width + 2 * rope
    depth = nd * tokens
    rows = heads * tokens
    scale = (NOPE + rope) ** (-0.5)
    paired = spacing == [0, 1, 2, 3, 4] and blocks % 2 == 0

    hbm = pl.BlockSpec(memory_space=pltpu.HBM)
    vmem = pl.BlockSpec(memory_space=pltpu.VMEM)
    queries = pl.pallas_call(
        functools.partial(stage_kernel, (heads, tokens, width, rope)),
        in_specs=[hbm] * 3,
        out_specs=[vmem] * 2,
        out_shape=[
            jax.ShapeDtypeStruct((rows, wide), BF16),
            jax.ShapeDtypeStruct((rows, width), BF16),
        ],
        scratch_shapes=[
            pltpu.VMEM((tokens, heads * rope), BF16),
            pltpu.SemaphoreType.DMA((2 * heads + 1,)),
        ],
        cost_estimate=pl.CostEstimate(
            flops=2 * rows * wide * width, bytes_accessed=8 * rows * wide, transcendentals=0
        ),
        compiler_params=pltpu.CompilerParams(vmem_limit_bytes=VMEM),
        name="stage",
    )(query_latent, query_rotary, upstream)

    own = jnp.concatenate([latent, key_rotary, key_rotary], axis=1)
    gathered = [own] + [rotated(own, "inner", k) for k in range(1, inner)]
    gathered, queries = lax.optimization_barrier((gathered, queries))
    near = jnp.concatenate(gathered, axis=0)
    if paired:
        order = [2, 4, 0, 1, 3]
        kept = 3
        two, four = rotated(near, "blk", 2), rotated(near, "blk", 4)
        sources = [(0,), (1,), (2,), (4, 3), (5, 4)]
        key_arrays = [two, four, near, swapped(near), swapped(two), swapped(four)]
    else:
        order = spacing
        kept = 1
        sources = [(d,) for d in range(nd)]
        key_arrays = [near] + [rotated(near, "blk", d) for d in spacing[1:]]
    sent = nd - kept
    entries = [spacing.index(d) for d in order]

    ds, weights, keys, grads = pl.pallas_call(
        functools.partial(
            scores_kernel, (nd, kept, pairs, tokens, shard, width, rope, scale), sources, entries
        ),
        in_specs=[pl.BlockSpec(memory_space=pltpu.SMEM)] + [vmem] * (2 + len(key_arrays)),
        out_specs=[vmem] * 4,
        out_shape=[
            jax.ShapeDtypeStruct((depth, rows), BF16),
            jax.ShapeDtypeStruct((kept * tokens, rows), BF16),
            jax.ShapeDtypeStruct((depth, wide), BF16),
            jax.ShapeDtypeStruct((sent * tokens, wide), BF16),
        ],
        scratch_shapes=[
            pltpu.VMEM((2, depth, 2 * tokens), F32),
            pltpu.VMEM((2, depth, 2 * tokens), F32),
            pltpu.VMEM((sent * tokens, rows), BF16),
        ],
        cost_estimate=pl.CostEstimate(
            flops=2 * rows * (depth + sent * tokens) * (wide + width),
            bytes_accessed=2 * rows * (2 * wide + depth),
            transcendentals=rows * depth,
        ),
        compiler_params=pltpu.CompilerParams(vmem_limit_bytes=VMEM),
        name="scores",
    )(pattern, *queries, *key_arrays)

    if paired:
        met = swapped(grads)
        late = pl.pallas_call(
            functools.partial(gradient_kernel, ((kept - 1) * tokens, width)),
            out_shape=jax.ShapeDtypeStruct(((kept - 1) * tokens, wide), F32),
            cost_estimate=pl.CostEstimate(
                flops=2 * rows * (kept - 1) * tokens * (wide + width),
                bytes_accessed=4 * rows * wide,
                transcendentals=0,
            ),
            compiler_params=pltpu.CompilerParams(vmem_limit_bytes=VMEM),
            name="late_gradients",
        )(ds, weights, *queries)
        to_two, to_four = pl.pallas_call(
            merge_kernel,
            out_shape=[jax.ShapeDtypeStruct((tokens, wide), BF16)] * 2,
            compiler_params=pltpu.CompilerParams(vmem_limit_bytes=VMEM),
            name="merge",
        )(late, met)
        back = [rotated(to_two, "blk", -2), rotated(to_four, "blk", -4)]
        handed = [met]
    else:
        back = [
            rotated(grads[k * tokens : (k + 1) * tokens], "blk", -d)
            for k, d in enumerate(spacing[1:])
        ]
        handed = []

    own_grad, query_cotangent, rotary_cotangent = pl.pallas_call(
        functools.partial(own_kernel, (kept - 1, pairs, tokens, width, rope)),
        in_specs=[vmem] * (5 + len(handed)),
        out_specs=[vmem, hbm, hbm],
        out_shape=[
            jax.ShapeDtypeStruct((tokens, wide), F32),
            jax.ShapeDtypeStruct(query_latent.shape, BF16),
            jax.ShapeDtypeStruct(query_rotary.shape, BF16),
        ],
        scratch_shapes=[
            pltpu.VMEM(query_latent.shape, BF16),
            pltpu.VMEM(query_rotary.shape, BF16),
            pltpu.SemaphoreType.DMA((pairs + 1,)),
        ],
        cost_estimate=pl.CostEstimate(
            flops=2 * rows * (tokens * (wide + width) + depth * wide),
            bytes_accessed=2 * rows * (wide + depth),
            transcendentals=0,
        ),
        compiler_params=pltpu.CompilerParams(vmem_limit_bytes=VMEM),
        name="own_gradients",
    )(ds, weights, *queries, keys, *handed)

    parts = pl.pallas_call(
        functools.partial(total_kernel, len(back)),
        out_shape=[
            jax.ShapeDtypeStruct((shard, wide), F32 if k == 0 else BF16) for k in range(inner)
        ],
        compiler_params=pltpu.CompilerParams(vmem_limit_bytes=VMEM),
        name="total",
    )(own_grad, *back)
    moved = [rotated(parts[k], "inner", -k) for k in range(1, inner)]

    latent_cotangent, positional_cotangent = pl.pallas_call(
        functools.partial(finish_kernel, (width, rope)),
        out_shape=[
            jax.ShapeDtypeStruct((shard, width), F32),
            jax.ShapeDtypeStruct((shard, rope), F32),
        ],
        compiler_params=pltpu.CompilerParams(vmem_limit_bytes=VMEM),
        name="finish",
    )(parts[0], *moved)
    return (query_cotangent, rotary_cotangent, latent_cotangent, positional_cotangent)


def solution(mesh):
    in_specs = (
        P("blk", "inner"),
        P("blk", "inner"),
        P("blk", "inner"),
        P(("blk", "inner"), None),
        P(("blk", "inner"), None),
        P("blk", None),
    )
    out_specs = (
        P("blk", "inner"),
        P("blk", "inner"),
        P(("blk", "inner"), None),
        P(("blk", "inner"), None),
    )
    return jax.shard_map(
        per_device, mesh=mesh, in_specs=in_specs, out_specs=out_specs, check_vma=False
    )
```

```python
import functools

import jax
import jax.numpy as jnp
from jax import lax
from jax.experimental import pallas as pl
from jax.experimental.pallas import tpu as pltpu
from jax.sharding import PartitionSpec as P


NOPE = 128
WIN = 2
NSTR = 4
LOG2E = 1.4426950408889634
FLOOR = -1e30
BF16 = jnp.bfloat16
F32 = jnp.float32
VMEM = 24 * 1024 * 1024


def spacing_list(blocks):
    spacing = blocks // 8
    listed = set(range(WIN))
    for number in range(1, NSTR + 1):
        listed.add(number * spacing)
    return sorted(listed)


def rotated(value, axis, steps):
    count = lax.axis_size(axis)
    return lax.ppermute(value, axis, [(s, (s + steps) % count) for s in range(count)])


def swapped(value):
    count = lax.axis_size("blk")
    return lax.ppermute(value, "blk", [(s, s + 1 - 2 * (s % 2)) for s in range(count)])


def stacked_rope(rope_pair, rope):
    lane = lax.broadcasted_iota(jnp.int32, rope_pair.shape, 1)
    zero = jnp.zeros_like(rope_pair)
    return jnp.concatenate(
        [jnp.where(lane < rope, rope_pair, zero), jnp.where(lane >= rope, rope_pair, zero)], axis=0
    )


def stage_kernel(dims, x_ref, *refs):
    heads, tokens, latent, rope = dims
    *rope_refs, out_ref, sems = refs
    copies = []
    for h in range(heads):
        rows = slice(h * tokens, (h + 1) * tokens)
        cols = slice(h * latent, (h + 1) * latent)
        copies.append(
            pltpu.make_async_copy(x_ref.at[:, cols], out_ref.at[rows, :latent], sems.at[h])
        )
    for copy in copies:
        copy.start()
    for ref in rope_refs:
        for p in range(heads // 2):
            rows = slice(2 * p * tokens, 2 * (p + 1) * tokens)
            out_ref[rows, latent:] = stacked_rope(ref[:, 2 * p * rope : 2 * (p + 1) * rope], rope)
    for copy in copies:
        copy.wait()


def merge_kernel(late_ref, met_ref, four_ref, two_ref):
    tokens = two_ref.shape[0]
    odd = lax.rem(lax.axis_index("blk"), 2) == 1
    one, three = met_ref[:tokens].astype(F32), met_ref[tokens:].astype(F32)
    four_ref[...] = (late_ref[:tokens] + jnp.where(odd, three, 0.0)).astype(BF16)
    two_ref[...] = (late_ref[tokens:] + jnp.where(odd, one, three)).astype(BF16)


def total_kernel(returned, own_ref, *refs):
    total = own_ref[...]
    for ref in refs[:returned]:
        total += ref[...].astype(F32)
    for k, ref in enumerate(refs[returned:]):
        shard = ref.shape[0]
        ref[...] = total[k * shard : (k + 1) * shard].astype(ref.dtype)


def finish_kernel(dims, own_ref, *refs):
    latent, rope = dims
    *parts, latent_ref, rope_ref = refs
    total = own_ref[...]
    for part in parts:
        total += part[...].astype(F32)
    latent_ref[...] = total[:, :latent]
    rope_ref[...] = total[:, latent : latent + rope] + total[:, latent + rope :]


def key_gradient(ds, weights, q2, u2, latent):
    nn = (((1,), (0,)), ((), ()))
    part = lax.dot_general(ds, q2, nn, preferred_element_type=F32)
    mixed = lax.dot_general(weights, u2, nn, preferred_element_type=F32)
    return part[:, :latent] + mixed, part[:, latent:]


def place_keys(keys, key_refs, sources, tokens):
    odd = lax.rem(lax.axis_index("blk"), 2) == 1
    for d, source in enumerate(sources):
        block = key_refs[source[0]][...]
        if len(source) == 2:
            block = jnp.where(odd, key_refs[source[1]][...], block)
        keys[d * tokens : (d + 1) * tokens, :] = block


def products(keys, q2_ref, u2_ref, lanes, latent):
    nt = (((1,), (1,)), ((), ()))
    s = lax.dot_general(keys[...], q2_ref[lanes, :], nt, preferred_element_type=F32)
    p = lax.dot_general(keys[:, :latent], u2_ref[lanes, :], nt, preferred_element_type=F32)
    return s, p


def early_kernel(dims, sources, entries, pattern_ref, q2_ref, u2_ref, *refs):
    pairs, tokens, shard, latent, scale = dims
    e_ref, p_ref, stats_ref, keys = refs[-4:]
    place_keys(keys, refs[:-4], sources, tokens)
    row = lax.broadcasted_iota(jnp.int32, (tokens, 2 * tokens), 0)
    col = lax.broadcasted_iota(jnp.int32, (tokens, 2 * tokens), 1)
    slots = tokens // shard
    owner = lax.rem(lax.axis_index("inner") - row // shard + slots, slots)
    causal = owner * shard + lax.rem(row, shard) <= lax.rem(col, tokens)
    span = lambda p: slice(2 * p * tokens, 2 * (p + 1) * tokens)

    def fill(p):
        lanes = span(p)
        e_ref[:, lanes], p_ref[:, lanes] = products(keys, q2_ref, u2_ref, lanes, latent)

    fill(0)
    for p in range(pairs):
        if p + 1 < pairs:
            fill(p + 1)
        lanes = span(p)
        peak = None
        for d, entry in enumerate(entries):
            rows = slice(d * tokens, (d + 1) * tokens)
            allowed = pattern_ref[0, entry] >= 0
            if entry == 0:
                allowed = jnp.logical_and(causal, allowed)
            s = jnp.where(allowed, e_ref[rows, lanes] * (scale * LOG2E), -jnp.inf)
            e_ref[rows, lanes] = s
            top = jnp.max(s, axis=0, keepdims=True)
            peak = top if peak is None else jnp.maximum(peak, top)
        peak = jnp.maximum(peak, FLOOR)
        total = jnp.zeros_like(peak)
        mixed = jnp.zeros_like(peak)
        for d in range(len(entries)):
            rows = slice(d * tokens, (d + 1) * tokens)
            e = jnp.exp2(e_ref[rows, lanes] - peak)
            e_ref[rows, lanes] = e
            total += jnp.sum(e, axis=0, keepdims=True)
            mixed += jnp.sum(e * p_ref[rows, lanes], axis=0, keepdims=True)
        stats_ref[0:1, lanes] = peak
        stats_ref[1:2, lanes] = total
        stats_ref[2:3, lanes] = mixed


def scores_kernel(dims, groups, sources, entries, pattern_ref, q2_ref, u2_ref, *refs):
    nd, kept, pairs, tokens, latent, scale = dims
    early = [refs[3 * g : 3 * g + 3] for g in range(len(groups))]
    ds_ref, kept_ref, keys, grad_ref, tail, s_scr, t_scr, w_scr = refs[-8:]
    key_refs = refs[3 * len(groups) : -8]
    place_keys(keys, key_refs, sources, tokens)
    later = [d for d in range(nd) if not any(d in group for group in groups)]
    place_keys(tail, key_refs, [sources[d] for d in later], tokens)
    chosen = [pattern_ref[0, entries[d]] >= 0 for d in later]
    span = lambda p: slice(2 * p * tokens, 2 * (p + 1) * tokens)
    block = lambda k: slice(k * tokens, (k + 1) * tokens)

    def fill(p):
        s_scr[p % 2], t_scr[p % 2] = products(tail, q2_ref, u2_ref, span(p), latent)

    fill(0)
    for p in range(pairs):
        if p + 1 < pairs:
            fill(p + 1)
        lanes = span(p)
        slot = p % 2
        before = [stats_ref[0:1, lanes] for _, _, stats_ref in early]
        peak = functools.reduce(jnp.maximum, before)
        for k in range(len(later)):
            s = jnp.where(chosen[k], s_scr[slot, block(k), :] * (scale * LOG2E), -jnp.inf)
            s_scr[slot, block(k), :] = s
            peak = jnp.maximum(peak, jnp.max(s, axis=0, keepdims=True))
        shrink = [jnp.exp2(b - peak) for b in before]
        total = sum(f * refs3[2][1:2, lanes] for f, refs3 in zip(shrink, early))
        mixed = sum(f * refs3[2][2:3, lanes] for f, refs3 in zip(shrink, early))
        for k in range(len(later)):
            e = jnp.exp2(s_scr[slot, block(k), :] - peak)
            s_scr[slot, block(k), :] = e
            total += jnp.sum(e, axis=0, keepdims=True)
            mixed += jnp.sum(e * t_scr[slot, block(k), :], axis=0, keepdims=True)
        inverse = 1.0 / total
        correction = mixed * inverse
        factors = [f * inverse for f in shrink]
        for d in range(nd):
            if d in later:
                k = later.index(d)
                e, dp, factor = s_scr[slot, block(k), :], t_scr[slot, block(k), :], inverse
            else:
                g = [d in group for group in groups].index(True)
                source = block(groups[g].index(d))
                e, dp, factor = early[g][0][source, lanes], early[g][1][source, lanes], factors[g]
            w = (e * factor).astype(BF16)
            if d < kept:
                kept_ref[block(d), lanes] = w
            else:
                w_scr[block(d - kept), lanes] = w
            ds_ref[block(d), lanes] = (e * (factor * scale) * (dp - correction)).astype(BF16)
    main, turned = key_gradient(
        ds_ref[kept * tokens :, :], w_scr[...], q2_ref[...], u2_ref[...], latent
    )
    grad_ref[:, :latent] = main.astype(BF16)
    grad_ref[:, latent:] = turned.astype(BF16)


def gradient_kernel(dims, ds_ref, w_ref, q2_ref, u2_ref, grad_ref):
    late, latent = dims
    main, turned = key_gradient(
        ds_ref[:late, :], w_ref[:late, :], q2_ref[...], u2_ref[...], latent
    )
    grad_ref[:, :latent] = main
    grad_ref[:, latent:] = turned


def own_kernel(dims, ds_ref, w_ref, q2_ref, u2_ref, keys_ref, *refs):
    own, pairs, tokens, latent, rope = dims
    *met_refs, grad_ref, dq_ref, dr_ref, dq_scr, dr_scr, sems = refs
    tn = (((0,), (0,)), ((), ()))
    lane = lax.broadcasted_iota(jnp.int32, (tokens, 2 * rope), 1)
    copies = []
    for p in range(pairs):
        lanes = slice(2 * p * tokens, 2 * (p + 1) * tokens)
        dq = lax.dot_general(ds_ref[:, lanes], keys_ref[...], tn, preferred_element_type=F32)
        even, odd = dq[:tokens], dq[tokens:]
        out = 2 * p * latent
        dq_scr[:, out : out + latent] = even[:, :latent].astype(BF16)
        dq_scr[:, out + latent : out + 2 * latent] = odd[:, :latent].astype(BF16)
        turned = jnp.where(lane < rope, even[:, latent:], odd[:, latent:])
        dr_scr[:, 2 * p * rope : 2 * (p + 1) * rope] = turned.astype(BF16)
        cols = slice(out, out + 2 * latent)
        copies.append(pltpu.make_async_copy(dq_scr.at[:, cols], dq_ref.at[:, cols], sems.at[p]))
        copies[-1].start()
    copies.append(pltpu.make_async_copy(dr_scr, dr_ref, sems.at[pairs]))
    copies[-1].start()
    rows = slice(own * tokens, (own + 1) * tokens)
    main, turned = key_gradient(
        ds_ref[rows, :], w_ref[rows, :], q2_ref[...], u2_ref[...], latent
    )
    start = jnp.zeros(grad_ref.shape, F32)
    for ref in met_refs:
        is_odd = lax.rem(lax.axis_index("blk"), 2) == 1
        start = jnp.where(is_odd, start, ref[:tokens, :].astype(F32))
    grad_ref[:, :latent] = start[:, :latent] + main
    grad_ref[:, latent:] = start[:, latent:] + turned
    for copy in copies:
        copy.wait()


def per_device(query_latent, query_rotary, upstream, latent, key_rotary, pattern):
    blocks = lax.axis_size("blk")
    spacing = spacing_list(blocks)
    nd = len(spacing)
    inner = lax.axis_size("inner")
    tokens = query_latent.shape[0]
    shard, width = latent.shape
    rope = key_rotary.shape[1]
    heads = query_latent.shape[1] // width
    pairs = heads // 2
    wide = width + 2 * rope
    depth = nd * tokens
    rows = heads * tokens
    scale = (NOPE + rope) ** (-0.5)
    paired = spacing == [0, 1, 2, 3, 4] and blocks % 2 == 0

    hbm = pl.BlockSpec(memory_space=pltpu.HBM)
    vmem = pl.BlockSpec(memory_space=pltpu.VMEM)
    smem = pl.BlockSpec(memory_space=pltpu.SMEM)
    params = pltpu.CompilerParams(vmem_limit_bytes=VMEM)

    def staged(lanes, array, *ropes):
        return pl.pallas_call(
            functools.partial(stage_kernel, (heads, tokens, width, rope)),
            in_specs=[hbm] + [vmem] * len(ropes),
            out_specs=vmem,
            out_shape=jax.ShapeDtypeStruct((rows, lanes), BF16),
            scratch_shapes=[pltpu.SemaphoreType.DMA((heads,))],
            cost_estimate=pl.CostEstimate(
                flops=rows * lanes * width, bytes_accessed=4 * rows * lanes, transcendentals=0
            ),
            compiler_params=params,
        )(array, *ropes)

    q2 = staged(wide, query_latent, query_rotary)
    own = jnp.concatenate([latent, key_rotary, key_rotary], axis=1)
    gathered = [own] + [rotated(own, "inner", k) for k in range(1, inner)]
    gathered, q2 = lax.optimization_barrier((gathered, q2))
    near = jnp.concatenate(gathered, axis=0)
    u2 = staged(width, upstream)
    if paired:
        order = [4, 2, 0, 1, 3]
        kept = 3
        groups = [[1, 2], [0, 3]]
        two = rotated(near, "blk", 2)
        four = rotated(near, "blk", 4)
        near_met = swapped(near)
        two, u2 = lax.optimization_barrier((two, u2))
        two_met = swapped(two)
        sources = [(2,), (1,), (0,), (4, 3), (5, 4)]
    else:
        order = spacing
        kept = 1
        groups = [[0]]
        sources = [(d,) for d in range(nd)]
    sent = nd - kept
    entries = [spacing.index(d) for d in order]
    behind = depth - sum(len(group) for group in groups) * tokens

    def early_scores(group, key_arrays, sources):
        ahead = len(group) * tokens
        return pl.pallas_call(
            functools.partial(
                early_kernel,
                (pairs, tokens, shard, width, scale),
                sources,
                [entries[d] for d in group],
            ),
            in_specs=[smem] + [vmem] * (2 + len(key_arrays)),
            out_specs=[vmem] * 3,
            out_shape=[
                jax.ShapeDtypeStruct((ahead, rows), F32),
                jax.ShapeDtypeStruct((ahead, rows), F32),
                jax.ShapeDtypeStruct((8, rows), F32),
            ],
            scratch_shapes=[pltpu.VMEM((ahead, wide), BF16)],
            cost_estimate=pl.CostEstimate(
                flops=2 * rows * ahead * (wide + width),
                bytes_accessed=8 * rows * ahead,
                transcendentals=rows * ahead,
            ),
            compiler_params=params,
        )(pattern, q2, u2, *key_arrays)

    if paired:
        first = early_scores(groups[0], [two, near], [(0,), (1,)])
        four, first = lax.optimization_barrier((four, first))
        four_met = swapped(four)
        second = early_scores(groups[1], [four, near_met, two_met], [(0,), (2, 1)])
        early = [*first, *second]
        key_arrays = [near, two, four, near_met, two_met, four_met]
    else:
        early = early_scores(groups[0], [near], [(0,)])
        key_arrays = [near] + [rotated(near, "blk", d) for d in spacing[1:]]
    queries = (q2, u2)

    ds, weights, keys, grads = pl.pallas_call(
        functools.partial(
            scores_kernel, (nd, kept, pairs, tokens, width, scale), groups, sources, entries
        ),
        in_specs=[smem] + [vmem] * (2 + len(early) + len(key_arrays)),
        out_specs=[vmem] * 4,
        out_shape=[
            jax.ShapeDtypeStruct((depth, rows), BF16),
            jax.ShapeDtypeStruct((kept * tokens, rows), BF16),
            jax.ShapeDtypeStruct((depth, wide), BF16),
            jax.ShapeDtypeStruct((sent * tokens, wide), BF16),
        ],
        scratch_shapes=[
            pltpu.VMEM((behind, wide), BF16),
            pltpu.VMEM((2, behind, 2 * tokens), F32),
            pltpu.VMEM((2, behind, 2 * tokens), F32),
            pltpu.VMEM((sent * tokens, rows), BF16),
        ],
        cost_estimate=pl.CostEstimate(
            flops=2 * rows * (behind + sent * tokens) * (wide + width),
            bytes_accessed=8 * rows * depth,
            transcendentals=rows * behind,
        ),
        compiler_params=params,
        name="scores",
    )(pattern, *queries, *early, *key_arrays)

    if paired:
        met = swapped(grads)
        late = pl.pallas_call(
            functools.partial(gradient_kernel, ((kept - 1) * tokens, width)),
            out_shape=jax.ShapeDtypeStruct(((kept - 1) * tokens, wide), F32),
            cost_estimate=pl.CostEstimate(
                flops=2 * rows * (kept - 1) * tokens * (wide + width),
                bytes_accessed=4 * rows * wide,
                transcendentals=0,
            ),
            compiler_params=params,
            name="late_gradients",
        )(ds, weights, *queries)
        to_four, to_two = pl.pallas_call(
            merge_kernel,
            out_shape=[jax.ShapeDtypeStruct((tokens, wide), BF16)] * 2,
            compiler_params=params,
            name="merge",
        )(late, met)
        back = [rotated(to_two, "blk", -2), rotated(to_four, "blk", -4)]
        handed = [met]
    else:
        back = [
            rotated(grads[k * tokens : (k + 1) * tokens], "blk", -d)
            for k, d in enumerate(spacing[1:])
        ]
        handed = []

    own_grad, query_cotangent, rotary_cotangent = pl.pallas_call(
        functools.partial(own_kernel, (kept - 1, pairs, tokens, width, rope)),
        in_specs=[vmem] * (5 + len(handed)),
        out_specs=[vmem, hbm, hbm],
        out_shape=[
            jax.ShapeDtypeStruct((tokens, wide), F32),
            jax.ShapeDtypeStruct(query_latent.shape, BF16),
            jax.ShapeDtypeStruct(query_rotary.shape, BF16),
        ],
        scratch_shapes=[
            pltpu.VMEM(query_latent.shape, BF16),
            pltpu.VMEM(query_rotary.shape, BF16),
            pltpu.SemaphoreType.DMA((pairs + 1,)),
        ],
        cost_estimate=pl.CostEstimate(
            flops=2 * rows * (tokens * (wide + width) + depth * wide),
            bytes_accessed=2 * rows * (wide + depth),
            transcendentals=0,
        ),
        compiler_params=params,
        name="own_gradients",
    )(ds, weights, *queries, keys, *handed)

    parts = pl.pallas_call(
        functools.partial(total_kernel, len(back)),
        out_shape=[
            jax.ShapeDtypeStruct((shard, wide), F32 if k == 0 else BF16) for k in range(inner)
        ],
        compiler_params=params,
        name="total",
    )(own_grad, *back)
    moved = [rotated(parts[k], "inner", -k) for k in range(1, inner)]

    latent_cotangent, positional_cotangent = pl.pallas_call(
        functools.partial(finish_kernel, (width, rope)),
        out_shape=[
            jax.ShapeDtypeStruct((shard, width), F32),
            jax.ShapeDtypeStruct((shard, rope), F32),
        ],
        compiler_params=params,
        name="finish",
    )(parts[0], *moved)
    return (query_cotangent, rotary_cotangent, latent_cotangent, positional_cotangent)


def solution(mesh):
    in_specs = (
        P("blk", "inner"),
        P("blk", "inner"),
        P("blk", "inner"),
        P(("blk", "inner"), None),
        P(("blk", "inner"), None),
        P("blk", None),
    )
    out_specs = (
        P("blk", "inner"),
        P("blk", "inner"),
        P(("blk", "inner"), None),
        P(("blk", "inner"), None),
    )

    return jax.shard_map(per_device, mesh=mesh, in_specs=in_specs, out_specs=out_specs, check_vma=False)
```

```python
import functools

import jax
import jax.numpy as jnp
from jax import lax
from jax.experimental import pallas as pl
from jax.experimental.pallas import tpu as pltpu
from jax.sharding import PartitionSpec as P


NOPE = 128
WIN = 2
NSTR = 4
LOG2E = 1.4426950408889634
FLOOR = -1e30
BF16 = jnp.bfloat16
F32 = jnp.float32
VMEM = 24 * 1024 * 1024


def spacing_list(blocks):
    spacing = blocks // 8
    listed = set(range(WIN))
    for number in range(1, NSTR + 1):
        listed.add(number * spacing)
    return sorted(listed)


def rotated(value, axis, steps):
    count = lax.axis_size(axis)
    return lax.ppermute(value, axis, [(s, (s + steps) % count) for s in range(count)])


def swapped(value):
    count = lax.axis_size("blk")
    return lax.ppermute(value, "blk", [(s, s + 1 - 2 * (s % 2)) for s in range(count)])


def stacked_rope(rope_pair, rope):
    lane = lax.broadcasted_iota(jnp.int32, rope_pair.shape, 1)
    zero = jnp.zeros_like(rope_pair)
    return jnp.concatenate(
        [jnp.where(lane < rope, rope_pair, zero), jnp.where(lane >= rope, rope_pair, zero)], axis=0
    )


def stage_kernel(dims, x_ref, *refs):
    heads, tokens, latent, rope = dims
    *rope_refs, out_ref, sems = refs
    copies = []
    for h in range(heads):
        rows = slice(h * tokens, (h + 1) * tokens)
        cols = slice(h * latent, (h + 1) * latent)
        copies.append(
            pltpu.make_async_copy(x_ref.at[:, cols], out_ref.at[rows, :latent], sems.at[h])
        )
    for copy in copies:
        copy.start()
    for ref in rope_refs:
        for p in range(heads // 2):
            rows = slice(2 * p * tokens, 2 * (p + 1) * tokens)
            out_ref[rows, latent:] = stacked_rope(ref[:, 2 * p * rope : 2 * (p + 1) * rope], rope)
    for copy in copies:
        copy.wait()


def merge_kernel(late_ref, met_ref, two_ref, *four_refs):
    tokens = two_ref.shape[0]
    odd = lax.rem(lax.axis_index("blk"), 2) == 1
    one, three = met_ref[:tokens].astype(F32), met_ref[tokens:].astype(F32)
    two_ref[...] = (late_ref[tokens:] + jnp.where(odd, one, three)).astype(BF16)
    four = late_ref[:tokens] + jnp.where(odd, three, 0.0)
    for k, ref in enumerate(four_refs):
        shard = ref.shape[0]
        ref[...] = four[k * shard : (k + 1) * shard].astype(ref.dtype)


def sum_kernel(first_ref, *refs):
    *part_refs, out_ref = refs
    total = first_ref[...]
    for ref in part_refs:
        total += ref[...].astype(F32)
    out_ref[...] = total.astype(out_ref.dtype)


def total_kernel(returned, own_ref, *refs):
    total = own_ref[...]
    for ref in refs[:returned]:
        total += ref[...].astype(F32)
    for k, ref in enumerate(refs[returned:]):
        shard = ref.shape[0]
        ref[...] = total[k * shard : (k + 1) * shard].astype(ref.dtype)


def finish_kernel(dims, own_ref, *refs):
    latent, rope = dims
    *parts, latent_ref, rope_ref = refs
    total = own_ref[...]
    for part in parts:
        total += part[...].astype(F32)
    latent_ref[...] = total[:, :latent]
    rope_ref[...] = total[:, latent : latent + rope] + total[:, latent + rope :]


def key_gradient(ds, weights, q2, u2, latent):
    nn = (((1,), (0,)), ((), ()))
    part = lax.dot_general(ds, q2, nn, preferred_element_type=F32)
    mixed = lax.dot_general(weights, u2, nn, preferred_element_type=F32)
    return part[:, :latent] + mixed, part[:, latent:]


def place_keys(keys, key_refs, sources, tokens):
    odd = lax.rem(lax.axis_index("blk"), 2) == 1
    for d, source in enumerate(sources):
        block = key_refs[source[0]][...]
        if len(source) == 2:
            block = jnp.where(odd, key_refs[source[1]][...], block)
        keys[d * tokens : (d + 1) * tokens, :] = block


def products(keys, q2_ref, u2_ref, lanes, latent):
    nt = (((1,), (1,)), ((), ()))
    s = lax.dot_general(keys[...], q2_ref[lanes, :], nt, preferred_element_type=F32)
    p = lax.dot_general(keys[:, :latent], u2_ref[lanes, :], nt, preferred_element_type=F32)
    return s, p


def early_kernel(dims, sources, entries, pattern_ref, q2_ref, u2_ref, *refs):
    pairs, tokens, shard, latent, scale = dims
    e_ref, p_ref, stats_ref, keys = refs[-4:]
    place_keys(keys, refs[:-4], sources, tokens)
    row = lax.broadcasted_iota(jnp.int32, (tokens, 2 * tokens), 0)
    col = lax.broadcasted_iota(jnp.int32, (tokens, 2 * tokens), 1)
    slots = tokens // shard
    owner = lax.rem(lax.axis_index("inner") - row // shard + slots, slots)
    causal = owner * shard + lax.rem(row, shard) <= lax.rem(col, tokens)
    span = lambda p: slice(2 * p * tokens, 2 * (p + 1) * tokens)

    def fill(p):
        lanes = span(p)
        e_ref[:, lanes], p_ref[:, lanes] = products(keys, q2_ref, u2_ref, lanes, latent)

    fill(0)
    for p in range(pairs):
        if p + 1 < pairs:
            fill(p + 1)
        lanes = span(p)
        peak = None
        for d, entry in enumerate(entries):
            rows = slice(d * tokens, (d + 1) * tokens)
            allowed = pattern_ref[0, entry] >= 0
            if entry == 0:
                allowed = jnp.logical_and(causal, allowed)
            s = jnp.where(allowed, e_ref[rows, lanes] * (scale * LOG2E), -jnp.inf)
            e_ref[rows, lanes] = s
            top = jnp.max(s, axis=0, keepdims=True)
            peak = top if peak is None else jnp.maximum(peak, top)
        peak = jnp.maximum(peak, FLOOR)
        total = jnp.zeros_like(peak)
        mixed = jnp.zeros_like(peak)
        for d in range(len(entries)):
            rows = slice(d * tokens, (d + 1) * tokens)
            e = jnp.exp2(e_ref[rows, lanes] - peak)
            e_ref[rows, lanes] = e
            total += jnp.sum(e, axis=0, keepdims=True)
            mixed += jnp.sum(e * p_ref[rows, lanes], axis=0, keepdims=True)
        stats_ref[0:1, lanes] = peak
        stats_ref[1:2, lanes] = total
        stats_ref[2:3, lanes] = mixed


def scores_kernel(dims, groups, sources, entries, pattern_ref, q2_ref, u2_ref, *refs):
    nd, kept, pairs, tokens, latent, scale = dims
    early = [refs[3 * g : 3 * g + 3] for g in range(len(groups))]
    ds_ref, kept_ref, keys, grad_ref, tail, s_scr, t_scr, w_scr = refs[-8:]
    key_refs = refs[3 * len(groups) : -8]
    place_keys(keys, key_refs, sources, tokens)
    later = [d for d in range(nd) if not any(d in group for group in groups)]
    place_keys(tail, key_refs, [sources[d] for d in later], tokens)
    chosen = [pattern_ref[0, entries[d]] >= 0 for d in later]
    span = lambda p: slice(2 * p * tokens, 2 * (p + 1) * tokens)
    block = lambda k: slice(k * tokens, (k + 1) * tokens)

    def fill(p):
        s_scr[p % 2], t_scr[p % 2] = products(tail, q2_ref, u2_ref, span(p), latent)

    fill(0)
    for p in range(pairs):
        if p + 1 < pairs:
            fill(p + 1)
        lanes = span(p)
        slot = p % 2
        before = [stats_ref[0:1, lanes] for _, _, stats_ref in early]
        peak = functools.reduce(jnp.maximum, before)
        for k in range(len(later)):
            s = jnp.where(chosen[k], s_scr[slot, block(k), :] * (scale * LOG2E), -jnp.inf)
            s_scr[slot, block(k), :] = s
            peak = jnp.maximum(peak, jnp.max(s, axis=0, keepdims=True))
        shrink = [jnp.exp2(b - peak) for b in before]
        total = sum(f * refs3[2][1:2, lanes] for f, refs3 in zip(shrink, early))
        mixed = sum(f * refs3[2][2:3, lanes] for f, refs3 in zip(shrink, early))
        for k in range(len(later)):
            e = jnp.exp2(s_scr[slot, block(k), :] - peak)
            s_scr[slot, block(k), :] = e
            total += jnp.sum(e, axis=0, keepdims=True)
            mixed += jnp.sum(e * t_scr[slot, block(k), :], axis=0, keepdims=True)
        inverse = 1.0 / total
        correction = mixed * inverse
        factors = [f * inverse for f in shrink]
        for d in range(nd):
            if d in later:
                k = later.index(d)
                e, dp, factor = s_scr[slot, block(k), :], t_scr[slot, block(k), :], inverse
            else:
                g = [d in group for group in groups].index(True)
                source = block(groups[g].index(d))
                e, dp, factor = early[g][0][source, lanes], early[g][1][source, lanes], factors[g]
            w = (e * factor).astype(BF16)
            if d < kept:
                kept_ref[block(d), lanes] = w
            else:
                w_scr[block(d - kept), lanes] = w
            ds_ref[block(d), lanes] = (e * (factor * scale) * (dp - correction)).astype(BF16)
    main, turned = key_gradient(
        ds_ref[kept * tokens :, :], w_scr[...], q2_ref[...], u2_ref[...], latent
    )
    grad_ref[:, :latent] = main.astype(BF16)
    grad_ref[:, latent:] = turned.astype(BF16)


def gradient_kernel(dims, ds_ref, w_ref, q2_ref, u2_ref, grad_ref):
    late, latent = dims
    main, turned = key_gradient(
        ds_ref[:late, :], w_ref[:late, :], q2_ref[...], u2_ref[...], latent
    )
    grad_ref[:, :latent] = main
    grad_ref[:, latent:] = turned


def own_kernel(dims, ds_ref, w_ref, q2_ref, u2_ref, keys_ref, *refs):
    own, pairs, tokens, latent, rope = dims
    *met_refs, grad_ref, dq_ref, dr_ref, dq_scr, dr_scr, sems = refs
    tn = (((0,), (0,)), ((), ()))
    lane = lax.broadcasted_iota(jnp.int32, (tokens, 2 * rope), 1)
    copies = []
    for p in range(pairs):
        lanes = slice(2 * p * tokens, 2 * (p + 1) * tokens)
        dq = lax.dot_general(ds_ref[:, lanes], keys_ref[...], tn, preferred_element_type=F32)
        even, odd = dq[:tokens], dq[tokens:]
        out = 2 * p * latent
        dq_scr[:, out : out + latent] = even[:, :latent].astype(BF16)
        dq_scr[:, out + latent : out + 2 * latent] = odd[:, :latent].astype(BF16)
        turned = jnp.where(lane < rope, even[:, latent:], odd[:, latent:])
        dr_scr[:, 2 * p * rope : 2 * (p + 1) * rope] = turned.astype(BF16)
        cols = slice(out, out + 2 * latent)
        copies.append(pltpu.make_async_copy(dq_scr.at[:, cols], dq_ref.at[:, cols], sems.at[p]))
        copies[-1].start()
    copies.append(pltpu.make_async_copy(dr_scr, dr_ref, sems.at[pairs]))
    copies[-1].start()
    rows = slice(own * tokens, (own + 1) * tokens)
    main, turned = key_gradient(
        ds_ref[rows, :], w_ref[rows, :], q2_ref[...], u2_ref[...], latent
    )
    start = jnp.zeros(grad_ref.shape, F32)
    for ref in met_refs:
        is_odd = lax.rem(lax.axis_index("blk"), 2) == 1
        start = jnp.where(is_odd, start, ref[:tokens, :].astype(F32))
    grad_ref[:, :latent] = start[:, :latent] + main
    grad_ref[:, latent:] = start[:, latent:] + turned
    for copy in copies:
        copy.wait()


def per_device(query_latent, query_rotary, upstream, latent, key_rotary, pattern):
    blocks = lax.axis_size("blk")
    spacing = spacing_list(blocks)
    nd = len(spacing)
    inner = lax.axis_size("inner")
    tokens = query_latent.shape[0]
    shard, width = latent.shape
    rope = key_rotary.shape[1]
    heads = query_latent.shape[1] // width
    pairs = heads // 2
    wide = width + 2 * rope
    depth = nd * tokens
    rows = heads * tokens
    scale = (NOPE + rope) ** (-0.5)
    paired = spacing == [0, 1, 2, 3, 4] and blocks % 2 == 0

    hbm = pl.BlockSpec(memory_space=pltpu.HBM)
    vmem = pl.BlockSpec(memory_space=pltpu.VMEM)
    smem = pl.BlockSpec(memory_space=pltpu.SMEM)
    params = pltpu.CompilerParams(vmem_limit_bytes=VMEM)

    def staged(lanes, array, *ropes):
        return pl.pallas_call(
            functools.partial(stage_kernel, (heads, tokens, width, rope)),
            in_specs=[hbm] + [vmem] * len(ropes),
            out_specs=vmem,
            out_shape=jax.ShapeDtypeStruct((rows, lanes), BF16),
            scratch_shapes=[pltpu.SemaphoreType.DMA((heads,))],
            cost_estimate=pl.CostEstimate(
                flops=rows * lanes * width, bytes_accessed=4 * rows * lanes, transcendentals=0
            ),
            compiler_params=params,
        )(array, *ropes)

    q2 = staged(wide, query_latent, query_rotary)
    own = jnp.concatenate([latent, key_rotary, key_rotary], axis=1)
    gathered = [own] + [rotated(own, "inner", k) for k in range(1, inner)]
    gathered, q2 = lax.optimization_barrier((gathered, q2))
    near = jnp.concatenate(gathered, axis=0)
    u2 = staged(width, upstream)
    if paired:
        order = [4, 2, 0, 1, 3]
        kept = 3
        groups = [[1, 2], [0, 3]]
        two = rotated(near, "blk", 2)
        four = rotated(near, "blk", 4)
        near_met = swapped(near)
        two, u2 = lax.optimization_barrier((two, u2))
        two_met = swapped(two)
        sources = [(2,), (1,), (0,), (4, 3), (5, 4)]
    else:
        order = spacing
        kept = 1
        groups = [[0]]
        sources = [(d,) for d in range(nd)]
    sent = nd - kept
    entries = [spacing.index(d) for d in order]
    behind = depth - sum(len(group) for group in groups) * tokens

    def early_scores(group, key_arrays, sources):
        ahead = len(group) * tokens
        return pl.pallas_call(
            functools.partial(
                early_kernel,
                (pairs, tokens, shard, width, scale),
                sources,
                [entries[d] for d in group],
            ),
            in_specs=[smem] + [vmem] * (2 + len(key_arrays)),
            out_specs=[vmem] * 3,
            out_shape=[
                jax.ShapeDtypeStruct((ahead, rows), F32),
                jax.ShapeDtypeStruct((ahead, rows), F32),
                jax.ShapeDtypeStruct((8, rows), F32),
            ],
            scratch_shapes=[pltpu.VMEM((ahead, wide), BF16)],
            cost_estimate=pl.CostEstimate(
                flops=2 * rows * ahead * (wide + width),
                bytes_accessed=8 * rows * ahead,
                transcendentals=rows * ahead,
            ),
            compiler_params=params,
        )(pattern, q2, u2, *key_arrays)

    if paired:
        first = early_scores(groups[0], [two, near], [(0,), (1,)])
        four, first = lax.optimization_barrier((four, first))
        four_met = swapped(four)
        second = early_scores(groups[1], [four, near_met, two_met], [(0,), (2, 1)])
        early = [*first, *second]
        key_arrays = [near, two, four, near_met, two_met, four_met]
    else:
        early = early_scores(groups[0], [near], [(0,)])
        key_arrays = [near] + [rotated(near, "blk", d) for d in spacing[1:]]
    queries = (q2, u2)

    ds, weights, keys, grads = pl.pallas_call(
        functools.partial(
            scores_kernel, (nd, kept, pairs, tokens, width, scale), groups, sources, entries
        ),
        in_specs=[smem] + [vmem] * (2 + len(early) + len(key_arrays)),
        out_specs=[vmem] * 4,
        out_shape=[
            jax.ShapeDtypeStruct((depth, rows), BF16),
            jax.ShapeDtypeStruct((kept * tokens, rows), BF16),
            jax.ShapeDtypeStruct((depth, wide), BF16),
            jax.ShapeDtypeStruct((sent * tokens, wide), BF16),
        ],
        scratch_shapes=[
            pltpu.VMEM((behind, wide), BF16),
            pltpu.VMEM((2, behind, 2 * tokens), F32),
            pltpu.VMEM((2, behind, 2 * tokens), F32),
            pltpu.VMEM((sent * tokens, rows), BF16),
        ],
        cost_estimate=pl.CostEstimate(
            flops=2 * rows * (behind + sent * tokens) * (wide + width),
            bytes_accessed=8 * rows * depth,
            transcendentals=rows * behind,
        ),
        compiler_params=params,
        name="scores",
    )(pattern, *queries, *early, *key_arrays)

    part_shapes = [
        jax.ShapeDtypeStruct((shard, wide), F32 if k == 0 else BF16) for k in range(inner)
    ]
    if paired:
        met = swapped(grads)
        late = pl.pallas_call(
            functools.partial(gradient_kernel, ((kept - 1) * tokens, width)),
            out_shape=jax.ShapeDtypeStruct(((kept - 1) * tokens, wide), F32),
            cost_estimate=pl.CostEstimate(
                flops=2 * rows * (kept - 1) * tokens * (wide + width),
                bytes_accessed=4 * rows * wide,
                transcendentals=0,
            ),
            compiler_params=params,
            name="late_gradients",
        )(ds, weights, *queries)
        to_two, *four_parts = pl.pallas_call(
            merge_kernel,
            out_shape=[jax.ShapeDtypeStruct((tokens, wide), BF16)] + part_shapes,
            compiler_params=params,
            name="merge",
        )(late, met)
        back = [rotated(to_two, "blk", -2)]
        four_moved = [rotated(four_parts[k], "inner", -k) for k in range(1, inner)]
        four_shard = pl.pallas_call(
            sum_kernel,
            out_shape=jax.ShapeDtypeStruct((shard, wide), BF16),
            compiler_params=params,
            name="sum_four",
        )(four_parts[0], *four_moved)
        shards_back = [rotated(four_shard, "blk", -4)]
        handed = [met]
    else:
        back = [
            rotated(grads[k * tokens : (k + 1) * tokens], "blk", -d)
            for k, d in enumerate(spacing[1:])
        ]
        handed = []
        shards_back = []

    own_grad, query_cotangent, rotary_cotangent = pl.pallas_call(
        functools.partial(own_kernel, (kept - 1, pairs, tokens, width, rope)),
        in_specs=[vmem] * (5 + len(handed)),
        out_specs=[vmem, hbm, hbm],
        out_shape=[
            jax.ShapeDtypeStruct((tokens, wide), F32),
            jax.ShapeDtypeStruct(query_latent.shape, BF16),
            jax.ShapeDtypeStruct(query_rotary.shape, BF16),
        ],
        scratch_shapes=[
            pltpu.VMEM(query_latent.shape, BF16),
            pltpu.VMEM(query_rotary.shape, BF16),
            pltpu.SemaphoreType.DMA((pairs + 1,)),
        ],
        cost_estimate=pl.CostEstimate(
            flops=2 * rows * (tokens * (wide + width) + depth * wide),
            bytes_accessed=2 * rows * (wide + depth),
            transcendentals=0,
        ),
        compiler_params=params,
        name="own_gradients",
    )(ds, weights, *queries, keys, *handed)

    parts = pl.pallas_call(
        functools.partial(total_kernel, len(back)),
        out_shape=part_shapes,
        compiler_params=params,
        name="total",
    )(own_grad, *back)
    moved = [rotated(parts[k], "inner", -k) for k in range(1, inner)]

    latent_cotangent, positional_cotangent = pl.pallas_call(
        functools.partial(finish_kernel, (width, rope)),
        out_shape=[
            jax.ShapeDtypeStruct((shard, width), F32),
            jax.ShapeDtypeStruct((shard, rope), F32),
        ],
        compiler_params=params,
        name="finish",
    )(parts[0], *moved, *shards_back)
    return (query_cotangent, rotary_cotangent, latent_cotangent, positional_cotangent)


def solution(mesh):
    in_specs = (
        P("blk", "inner"),
        P("blk", "inner"),
        P("blk", "inner"),
        P(("blk", "inner"), None),
        P(("blk", "inner"), None),
        P("blk", None),
    )
    out_specs = (
        P("blk", "inner"),
        P("blk", "inner"),
        P(("blk", "inner"), None),
        P(("blk", "inner"), None),
    )

    return jax.shard_map(per_device, mesh=mesh, in_specs=in_specs, out_specs=out_specs, check_vma=False)
```

```python
import functools

import jax
import jax.numpy as jnp
from jax import lax
from jax.experimental import pallas as pl
from jax.experimental.pallas import tpu as pltpu
from jax.sharding import PartitionSpec as P


NOPE = 128
WIN = 2
NSTR = 4
LOG2E = 1.4426950408889634
FLOOR = -1e30
BF16 = jnp.bfloat16
F32 = jnp.float32
VMEM = 24 * 1024 * 1024


def spacing_list(blocks):
    spacing = blocks // 8
    listed = set(range(WIN))
    for number in range(1, NSTR + 1):
        listed.add(number * spacing)
    return sorted(listed)


def rotated(value, axis, steps):
    count = lax.axis_size(axis)
    return lax.ppermute(value, axis, [(s, (s + steps) % count) for s in range(count)])


def swapped(value):
    count = lax.axis_size("blk")
    return lax.ppermute(value, "blk", [(s, s + 1 - 2 * (s % 2)) for s in range(count)])


def stacked_rope(rope_pair, rope):
    lane = lax.broadcasted_iota(jnp.int32, rope_pair.shape, 1)
    zero = jnp.zeros_like(rope_pair)
    return jnp.concatenate(
        [jnp.where(lane < rope, rope_pair, zero), jnp.where(lane >= rope, rope_pair, zero)], axis=0
    )


def stage_kernel(dims, x_ref, *refs):
    heads, tokens, latent, rope = dims
    *rope_refs, out_ref, sems = refs
    copies = []
    for h in range(heads):
        rows = slice(h * tokens, (h + 1) * tokens)
        cols = slice(h * latent, (h + 1) * latent)
        copies.append(
            pltpu.make_async_copy(x_ref.at[:, cols], out_ref.at[rows, :latent], sems.at[h])
        )
    for copy in copies:
        copy.start()
    for ref in rope_refs:
        for p in range(heads // 2):
            rows = slice(2 * p * tokens, 2 * (p + 1) * tokens)
            out_ref[rows, latent:] = stacked_rope(ref[:, 2 * p * rope : 2 * (p + 1) * rope], rope)
    for copy in copies:
        copy.wait()


def merge_kernel(late_ref, met_ref, two_ref, *four_refs):
    tokens = two_ref.shape[0]
    odd = lax.rem(lax.axis_index("blk"), 2) == 1
    one, three = met_ref[:tokens].astype(F32), met_ref[tokens:].astype(F32)
    two_ref[...] = (late_ref[tokens:] + jnp.where(odd, one, three)).astype(BF16)
    four = late_ref[:tokens] + jnp.where(odd, three, 0.0)
    for k, ref in enumerate(four_refs):
        shard = ref.shape[0]
        ref[...] = four[k * shard : (k + 1) * shard].astype(ref.dtype)


def sum_kernel(first_ref, *refs):
    *part_refs, out_ref = refs
    total = first_ref[...]
    for ref in part_refs:
        total += ref[...].astype(F32)
    out_ref[...] = total.astype(out_ref.dtype)


def total_kernel(returned, own_ref, *refs):
    total = own_ref[...]
    for ref in refs[:returned]:
        total += ref[...].astype(F32)
    for k, ref in enumerate(refs[returned:]):
        shard = ref.shape[0]
        ref[...] = total[k * shard : (k + 1) * shard].astype(ref.dtype)


def finish_kernel(dims, own_ref, *refs):
    latent, rope = dims
    *parts, latent_ref, rope_ref = refs
    total = own_ref[...]
    for part in parts:
        total += part[...].astype(F32)
    latent_ref[...] = total[:, :latent]
    rope_ref[...] = total[:, latent : latent + rope] + total[:, latent + rope :]


def key_gradient(ds, weights, q2, u2, latent):
    nn = (((1,), (0,)), ((), ()))
    part = lax.dot_general(ds, q2, nn, preferred_element_type=F32)
    mixed = lax.dot_general(weights, u2, nn, preferred_element_type=F32)
    return part[:, :latent] + mixed, part[:, latent:]


def place_keys(keys, key_refs, sources, tokens):
    odd = lax.rem(lax.axis_index("blk"), 2) == 1
    for d, source in enumerate(sources):
        block = key_refs[source[0]][...]
        if len(source) == 2:
            block = jnp.where(odd, key_refs[source[1]][...], block)
        keys[d * tokens : (d + 1) * tokens, :] = block


def products(keys, q2_ref, u2_ref, lanes, latent):
    nt = (((1,), (1,)), ((), ()))
    s = lax.dot_general(keys[...], q2_ref[lanes, :], nt, preferred_element_type=F32)
    p = lax.dot_general(keys[:, :latent], u2_ref[lanes, :], nt, preferred_element_type=F32)
    return s, p


def early_kernel(dims, sources, entries, pattern_ref, q2_ref, u2_ref, *refs):
    pairs, tokens, shard, latent, scale = dims
    e_ref, p_ref, stats_ref, keys = refs[-4:]
    place_keys(keys, refs[:-4], sources, tokens)
    row = lax.broadcasted_iota(jnp.int32, (tokens, 2 * tokens), 0)
    col = lax.broadcasted_iota(jnp.int32, (tokens, 2 * tokens), 1)
    slots = tokens // shard
    owner = lax.rem(lax.axis_index("inner") - row // shard + slots, slots)
    causal = owner * shard + lax.rem(row, shard) <= lax.rem(col, tokens)
    span = lambda p: slice(2 * p * tokens, 2 * (p + 1) * tokens)

    def fill(p):
        lanes = span(p)
        e_ref[:, lanes], p_ref[:, lanes] = products(keys, q2_ref, u2_ref, lanes, latent)

    fill(0)
    for p in range(pairs):
        if p + 1 < pairs:
            fill(p + 1)
        lanes = span(p)
        peak = None
        for d, entry in enumerate(entries):
            rows = slice(d * tokens, (d + 1) * tokens)
            allowed = pattern_ref[0, entry] >= 0
            if entry == 0:
                allowed = jnp.logical_and(causal, allowed)
            s = jnp.where(allowed, e_ref[rows, lanes] * (scale * LOG2E), -jnp.inf)
            e_ref[rows, lanes] = s
            top = jnp.max(s, axis=0, keepdims=True)
            peak = top if peak is None else jnp.maximum(peak, top)
        peak = jnp.maximum(peak, FLOOR)
        total = jnp.zeros_like(peak)
        mixed = jnp.zeros_like(peak)
        for d in range(len(entries)):
            rows = slice(d * tokens, (d + 1) * tokens)
            e = jnp.exp2(e_ref[rows, lanes] - peak)
            e_ref[rows, lanes] = e
            total += jnp.sum(e, axis=0, keepdims=True)
            mixed += jnp.sum(e * p_ref[rows, lanes], axis=0, keepdims=True)
        stats_ref[0:1, lanes] = peak
        stats_ref[1:2, lanes] = total
        stats_ref[2:3, lanes] = mixed


def scores_kernel(dims, groups, sources, entries, pattern_ref, q2_ref, u2_ref, *refs):
    nd, kept, pairs, tokens, latent, scale = dims
    early = [refs[3 * g : 3 * g + 3] for g in range(len(groups))]
    ds_ref, kept_ref, keys, grad_ref, tail, s_scr, t_scr, w_scr = refs[-8:]
    key_refs = refs[3 * len(groups) : -8]
    place_keys(keys, key_refs, sources, tokens)
    later = [d for d in range(nd) if not any(d in group for group in groups)]
    place_keys(tail, key_refs, [sources[d] for d in later], tokens)
    chosen = [pattern_ref[0, entries[d]] >= 0 for d in later]
    span = lambda p: slice(2 * p * tokens, 2 * (p + 1) * tokens)
    block = lambda k: slice(k * tokens, (k + 1) * tokens)

    def fill(p):
        s_scr[p % 2], t_scr[p % 2] = products(tail, q2_ref, u2_ref, span(p), latent)

    fill(0)
    for p in range(pairs):
        if p + 1 < pairs:
            fill(p + 1)
        lanes = span(p)
        slot = p % 2
        before = [stats_ref[0:1, lanes] for _, _, stats_ref in early]
        peak = functools.reduce(jnp.maximum, before)
        for k in range(len(later)):
            s = jnp.where(chosen[k], s_scr[slot, block(k), :] * (scale * LOG2E), -jnp.inf)
            s_scr[slot, block(k), :] = s
            peak = jnp.maximum(peak, jnp.max(s, axis=0, keepdims=True))
        shrink = [jnp.exp2(b - peak) for b in before]
        total = sum(f * refs3[2][1:2, lanes] for f, refs3 in zip(shrink, early))
        mixed = sum(f * refs3[2][2:3, lanes] for f, refs3 in zip(shrink, early))
        for k in range(len(later)):
            e = jnp.exp2(s_scr[slot, block(k), :] - peak)
            s_scr[slot, block(k), :] = e
            total += jnp.sum(e, axis=0, keepdims=True)
            mixed += jnp.sum(e * t_scr[slot, block(k), :], axis=0, keepdims=True)
        inverse = 1.0 / total
        correction = mixed * inverse
        factors = [f * inverse for f in shrink]
        for d in range(nd):
            if d in later:
                k = later.index(d)
                e, dp, factor = s_scr[slot, block(k), :], t_scr[slot, block(k), :], inverse
            else:
                g = [d in group for group in groups].index(True)
                source = block(groups[g].index(d))
                e, dp, factor = early[g][0][source, lanes], early[g][1][source, lanes], factors[g]
            w = (e * factor).astype(BF16)
            if d < kept:
                kept_ref[block(d), lanes] = w
            else:
                w_scr[block(d - kept), lanes] = w
            ds_ref[block(d), lanes] = (e * (factor * scale) * (dp - correction)).astype(BF16)
    main, turned = key_gradient(
        ds_ref[kept * tokens :, :], w_scr[...], q2_ref[...], u2_ref[...], latent
    )
    grad_ref[:, :latent] = main.astype(BF16)
    grad_ref[:, latent:] = turned.astype(BF16)


def gradient_kernel(dims, ds_ref, w_ref, q2_ref, u2_ref, grad_ref):
    late, latent = dims
    main, turned = key_gradient(
        ds_ref[:late, :], w_ref[:late, :], q2_ref[...], u2_ref[...], latent
    )
    grad_ref[:, :latent] = main
    grad_ref[:, latent:] = turned


def own_kernel(dims, ds_ref, w_ref, q2_ref, u2_ref, *refs):
    own, tokens, latent = dims
    *met_refs, grad_ref = refs
    rows = slice(own * tokens, (own + 1) * tokens)
    main, turned = key_gradient(
        ds_ref[rows, :], w_ref[rows, :], q2_ref[...], u2_ref[...], latent
    )
    start = jnp.zeros(grad_ref.shape, F32)
    for ref in met_refs:
        is_odd = lax.rem(lax.axis_index("blk"), 2) == 1
        start = jnp.where(is_odd, start, ref[:tokens, :].astype(F32))
    grad_ref[:, :latent] = start[:, :latent] + main
    grad_ref[:, latent:] = start[:, latent:] + turned


def query_kernel(dims, ds_ref, keys_ref, dq_ref, dr_ref, dq_scr, dr_scr, sems):
    pairs, tokens, latent, rope = dims
    tn = (((0,), (0,)), ((), ()))
    lane = lax.broadcasted_iota(jnp.int32, (tokens, 2 * rope), 1)
    copies = []
    for p in range(pairs):
        lanes = slice(2 * p * tokens, 2 * (p + 1) * tokens)
        dq = lax.dot_general(ds_ref[:, lanes], keys_ref[...], tn, preferred_element_type=F32)
        even, odd = dq[:tokens], dq[tokens:]
        out = 2 * p * latent
        dq_scr[:, out : out + latent] = even[:, :latent].astype(BF16)
        dq_scr[:, out + latent : out + 2 * latent] = odd[:, :latent].astype(BF16)
        turned = jnp.where(lane < rope, even[:, latent:], odd[:, latent:])
        dr_scr[:, 2 * p * rope : 2 * (p + 1) * rope] = turned.astype(BF16)
        cols = slice(out, out + 2 * latent)
        copies.append(pltpu.make_async_copy(dq_scr.at[:, cols], dq_ref.at[:, cols], sems.at[p]))
        copies[-1].start()
    copies.append(pltpu.make_async_copy(dr_scr, dr_ref, sems.at[pairs]))
    copies[-1].start()
    for copy in copies:
        copy.wait()


def per_device(query_latent, query_rotary, upstream, latent, key_rotary, pattern):
    blocks = lax.axis_size("blk")
    spacing = spacing_list(blocks)
    nd = len(spacing)
    inner = lax.axis_size("inner")
    tokens = query_latent.shape[0]
    shard, width = latent.shape
    rope = key_rotary.shape[1]
    heads = query_latent.shape[1] // width
    pairs = heads // 2
    wide = width + 2 * rope
    depth = nd * tokens
    rows = heads * tokens
    scale = (NOPE + rope) ** (-0.5)
    paired = spacing == [0, 1, 2, 3, 4] and blocks % 2 == 0

    hbm = pl.BlockSpec(memory_space=pltpu.HBM)
    vmem = pl.BlockSpec(memory_space=pltpu.VMEM)
    smem = pl.BlockSpec(memory_space=pltpu.SMEM)
    params = pltpu.CompilerParams(vmem_limit_bytes=VMEM)

    def staged(lanes, array, *ropes):
        return pl.pallas_call(
            functools.partial(stage_kernel, (heads, tokens, width, rope)),
            in_specs=[hbm] + [vmem] * len(ropes),
            out_specs=vmem,
            out_shape=jax.ShapeDtypeStruct((rows, lanes), BF16),
            scratch_shapes=[pltpu.SemaphoreType.DMA((heads,))],
            cost_estimate=pl.CostEstimate(
                flops=rows * lanes * width, bytes_accessed=4 * rows * lanes, transcendentals=0
            ),
            compiler_params=params,
        )(array, *ropes)

    q2 = staged(wide, query_latent, query_rotary)
    own = jnp.concatenate([latent, key_rotary, key_rotary], axis=1)
    gathered = [own] + [rotated(own, "inner", k) for k in range(1, inner)]
    gathered = lax.optimization_barrier(gathered)
    near = jnp.concatenate(gathered, axis=0)
    u2 = staged(width, upstream)
    if paired:
        order = [4, 2, 0, 1, 3]
        kept = 3
        groups = [[1, 2], [0, 3]]
        two = rotated(near, "blk", 2)
        four = rotated(near, "blk", 4)
        near_met = swapped(near)
        two, q2, u2 = lax.optimization_barrier((two, q2, u2))
        two_met = swapped(two)
        sources = [(2,), (1,), (0,), (4, 3), (5, 4)]
    else:
        order = spacing
        kept = 1
        groups = [[0]]
        sources = [(d,) for d in range(nd)]
    sent = nd - kept
    entries = [spacing.index(d) for d in order]
    behind = depth - sum(len(group) for group in groups) * tokens

    def early_scores(group, key_arrays, sources):
        ahead = len(group) * tokens
        return pl.pallas_call(
            functools.partial(
                early_kernel,
                (pairs, tokens, shard, width, scale),
                sources,
                [entries[d] for d in group],
            ),
            in_specs=[smem] + [vmem] * (2 + len(key_arrays)),
            out_specs=[vmem] * 3,
            out_shape=[
                jax.ShapeDtypeStruct((ahead, rows), F32),
                jax.ShapeDtypeStruct((ahead, rows), F32),
                jax.ShapeDtypeStruct((8, rows), F32),
            ],
            scratch_shapes=[pltpu.VMEM((ahead, wide), BF16)],
            cost_estimate=pl.CostEstimate(
                flops=2 * rows * ahead * (wide + width),
                bytes_accessed=8 * rows * ahead,
                transcendentals=rows * ahead,
            ),
            compiler_params=params,
        )(pattern, q2, u2, *key_arrays)

    if paired:
        first = early_scores(groups[0], [two, near], [(0,), (1,)])
        four, first = lax.optimization_barrier((four, first))
        four_met = swapped(four)
        second = early_scores(groups[1], [four, near_met, two_met], [(0,), (2, 1)])
        early = [*first, *second]
        key_arrays = [near, two, four, near_met, two_met, four_met]
    else:
        early = early_scores(groups[0], [near], [(0,)])
        key_arrays = [near] + [rotated(near, "blk", d) for d in spacing[1:]]
    queries = (q2, u2)

    ds, weights, keys, grads = pl.pallas_call(
        functools.partial(
            scores_kernel, (nd, kept, pairs, tokens, width, scale), groups, sources, entries
        ),
        in_specs=[smem] + [vmem] * (2 + len(early) + len(key_arrays)),
        out_specs=[vmem] * 4,
        out_shape=[
            jax.ShapeDtypeStruct((depth, rows), BF16),
            jax.ShapeDtypeStruct((kept * tokens, rows), BF16),
            jax.ShapeDtypeStruct((depth, wide), BF16),
            jax.ShapeDtypeStruct((sent * tokens, wide), BF16),
        ],
        scratch_shapes=[
            pltpu.VMEM((behind, wide), BF16),
            pltpu.VMEM((2, behind, 2 * tokens), F32),
            pltpu.VMEM((2, behind, 2 * tokens), F32),
            pltpu.VMEM((sent * tokens, rows), BF16),
        ],
        cost_estimate=pl.CostEstimate(
            flops=2 * rows * (behind + sent * tokens) * (wide + width),
            bytes_accessed=8 * rows * depth,
            transcendentals=rows * behind,
        ),
        compiler_params=params,
        name="scores",
    )(pattern, *queries, *early, *key_arrays)

    part_shapes = [
        jax.ShapeDtypeStruct((shard, wide), F32 if k == 0 else BF16) for k in range(inner)
    ]
    if paired:
        met = swapped(grads)
        late = pl.pallas_call(
            functools.partial(gradient_kernel, ((kept - 1) * tokens, width)),
            out_shape=jax.ShapeDtypeStruct(((kept - 1) * tokens, wide), F32),
            cost_estimate=pl.CostEstimate(
                flops=2 * rows * (kept - 1) * tokens * (wide + width),
                bytes_accessed=4 * rows * wide,
                transcendentals=0,
            ),
            compiler_params=params,
            name="late_gradients",
        )(ds, weights, *queries)
        to_two, *four_parts = pl.pallas_call(
            merge_kernel,
            out_shape=[jax.ShapeDtypeStruct((tokens, wide), BF16)] + part_shapes,
            compiler_params=params,
            name="merge",
        )(late, met)
        back = [rotated(to_two, "blk", -2)]
        four_moved = [rotated(four_parts[k], "inner", -k) for k in range(1, inner)]
        four_shard = pl.pallas_call(
            sum_kernel,
            out_shape=jax.ShapeDtypeStruct((shard, wide), BF16),
            compiler_params=params,
            name="sum_four",
        )(four_parts[0], *four_moved)
        shards_back = [rotated(four_shard, "blk", -4)]
        handed = [met]
    else:
        back = [
            rotated(grads[k * tokens : (k + 1) * tokens], "blk", -d)
            for k, d in enumerate(spacing[1:])
        ]
        handed = []
        shards_back = []

    own_grad = pl.pallas_call(
        functools.partial(own_kernel, (kept - 1, tokens, width)),
        out_shape=jax.ShapeDtypeStruct((tokens, wide), F32),
        cost_estimate=pl.CostEstimate(
            flops=2 * rows * tokens * (wide + width),
            bytes_accessed=2 * rows * wide,
            transcendentals=0,
        ),
        compiler_params=params,
        name="own_gradients",
    )(ds, weights, *queries, *handed)

    query_cotangent, rotary_cotangent = pl.pallas_call(
        functools.partial(query_kernel, (pairs, tokens, width, rope)),
        in_specs=[vmem] * 2,
        out_specs=[hbm] * 2,
        out_shape=[
            jax.ShapeDtypeStruct(query_latent.shape, BF16),
            jax.ShapeDtypeStruct(query_rotary.shape, BF16),
        ],
        scratch_shapes=[
            pltpu.VMEM(query_latent.shape, BF16),
            pltpu.VMEM(query_rotary.shape, BF16),
            pltpu.SemaphoreType.DMA((pairs + 1,)),
        ],
        cost_estimate=pl.CostEstimate(
            flops=2 * rows * depth * wide,
            bytes_accessed=2 * rows * (wide + depth),
            transcendentals=0,
        ),
        compiler_params=params,
        name="query_cotangents",
    )(ds, keys)

    parts = pl.pallas_call(
        functools.partial(total_kernel, len(back)),
        out_shape=part_shapes,
        compiler_params=params,
        name="total",
    )(own_grad, *back)
    moved = [rotated(parts[k], "inner", -k) for k in range(1, inner)]

    latent_cotangent, positional_cotangent = pl.pallas_call(
        functools.partial(finish_kernel, (width, rope)),
        out_shape=[
            jax.ShapeDtypeStruct((shard, width), F32),
            jax.ShapeDtypeStruct((shard, rope), F32),
        ],
        compiler_params=params,
        name="finish",
    )(parts[0], *moved, *shards_back)
    return (query_cotangent, rotary_cotangent, latent_cotangent, positional_cotangent)


def solution(mesh):
    in_specs = (
        P("blk", "inner"),
        P("blk", "inner"),
        P("blk", "inner"),
        P(("blk", "inner"), None),
        P(("blk", "inner"), None),
        P("blk", None),
    )
    out_specs = (
        P("blk", "inner"),
        P("blk", "inner"),
        P(("blk", "inner"), None),
        P(("blk", "inner"), None),
    )

    return jax.shard_map(per_device, mesh=mesh, in_specs=in_specs, out_specs=out_specs, check_vma=False)
```

```python
import functools

import jax
import jax.numpy as jnp
from jax import lax
from jax.experimental import pallas as pl
from jax.experimental.pallas import tpu as pltpu
from jax.sharding import PartitionSpec as P


NOPE = 128
WIN = 2
NSTR = 4
LOG2E = 1.4426950408889634
FLOOR = -1e30
BF16 = jnp.bfloat16
F32 = jnp.float32
VMEM = 24 * 1024 * 1024


def spacing_list(blocks):
    spacing = blocks // 8
    listed = set(range(WIN))
    for number in range(1, NSTR + 1):
        listed.add(number * spacing)
    return sorted(listed)


def rotated(value, axis, steps):
    count = lax.axis_size(axis)
    return lax.ppermute(value, axis, [(s, (s + steps) % count) for s in range(count)])


def swapped(value):
    count = lax.axis_size("blk")
    return lax.ppermute(value, "blk", [(s, s + 1 - 2 * (s % 2)) for s in range(count)])


def stacked_rope(rope_pair, rope):
    lane = lax.broadcasted_iota(jnp.int32, rope_pair.shape, 1)
    zero = jnp.zeros_like(rope_pair)
    return jnp.concatenate(
        [jnp.where(lane < rope, rope_pair, zero), jnp.where(lane >= rope, rope_pair, zero)], axis=0
    )


def stage_kernel(dims, x_ref, *refs):
    heads, tokens, latent, rope = dims
    *rope_refs, out_ref, sems = refs
    copies = []
    for h in range(heads):
        rows = slice(h * tokens, (h + 1) * tokens)
        cols = slice(h * latent, (h + 1) * latent)
        copies.append(
            pltpu.make_async_copy(x_ref.at[:, cols], out_ref.at[rows, :latent], sems.at[h])
        )
    for copy in copies:
        copy.start()
    for ref in rope_refs:
        for p in range(heads // 2):
            rows = slice(2 * p * tokens, 2 * (p + 1) * tokens)
            out_ref[rows, latent:] = stacked_rope(ref[:, 2 * p * rope : 2 * (p + 1) * rope], rope)
    for copy in copies:
        copy.wait()


def merge_kernel(late_ref, met_ref, two_ref, *four_refs):
    tokens = two_ref.shape[0]
    odd = lax.rem(lax.axis_index("blk"), 2) == 1
    one, three = met_ref[:tokens].astype(F32), met_ref[tokens:].astype(F32)
    two_ref[...] = (late_ref[tokens:] + jnp.where(odd, one, three)).astype(BF16)
    four = late_ref[:tokens] + jnp.where(odd, three, 0.0)
    for k, ref in enumerate(four_refs):
        shard = ref.shape[0]
        ref[...] = four[k * shard : (k + 1) * shard].astype(ref.dtype)


def sum_kernel(first_ref, *refs):
    *part_refs, out_ref = refs
    total = first_ref[...]
    for ref in part_refs:
        total += ref[...].astype(F32)
    out_ref[...] = total.astype(out_ref.dtype)


def total_kernel(returned, own_ref, *refs):
    total = own_ref[...]
    for ref in refs[:returned]:
        total += ref[...].astype(F32)
    for k, ref in enumerate(refs[returned:]):
        shard = ref.shape[0]
        ref[...] = total[k * shard : (k + 1) * shard].astype(ref.dtype)


def finish_kernel(dims, own_ref, *refs):
    latent, rope = dims
    *parts, latent_ref, rope_ref = refs
    total = own_ref[...]
    for part in parts:
        total += part[...].astype(F32)
    latent_ref[...] = total[:, :latent]
    rope_ref[...] = total[:, latent : latent + rope] + total[:, latent + rope :]


def key_gradient(ds, weights, q2, u2, latent):
    nn = (((1,), (0,)), ((), ()))
    part = lax.dot_general(ds, q2, nn, preferred_element_type=F32)
    mixed = lax.dot_general(weights, u2, nn, preferred_element_type=F32)
    return part[:, :latent] + mixed, part[:, latent:]


def place_keys(keys, key_refs, sources, tokens):
    odd = lax.rem(lax.axis_index("blk"), 2) == 1
    for d, source in enumerate(sources):
        block = key_refs[source[0]][...]
        if len(source) == 2:
            block = jnp.where(odd, key_refs[source[1]][...], block)
        keys[d * tokens : (d + 1) * tokens, :] = block


def products(keys, q2_ref, u2_ref, lanes, latent):
    nt = (((1,), (1,)), ((), ()))
    s = lax.dot_general(keys[...], q2_ref[lanes, :], nt, preferred_element_type=F32)
    p = lax.dot_general(keys[:, :latent], u2_ref[lanes, :], nt, preferred_element_type=F32)
    return s, p


def early_kernel(dims, sources, entries, pattern_ref, q2_ref, u2_ref, *refs):
    pairs, tokens, shard, latent, scale = dims
    e_ref, p_ref, stats_ref, keys = refs[-4:]
    place_keys(keys, refs[:-4], sources, tokens)
    row = lax.broadcasted_iota(jnp.int32, (tokens, 2 * tokens), 0)
    col = lax.broadcasted_iota(jnp.int32, (tokens, 2 * tokens), 1)
    slots = tokens // shard
    owner = lax.rem(lax.axis_index("inner") - row // shard + slots, slots)
    causal = owner * shard + lax.rem(row, shard) <= lax.rem(col, tokens)
    span = lambda p: slice(2 * p * tokens, 2 * (p + 1) * tokens)

    def fill(p):
        lanes = span(p)
        e_ref[:, lanes], p_ref[:, lanes] = products(keys, q2_ref, u2_ref, lanes, latent)

    fill(0)
    for p in range(pairs):
        if p + 1 < pairs:
            fill(p + 1)
        lanes = span(p)
        peak = None
        for d, entry in enumerate(entries):
            rows = slice(d * tokens, (d + 1) * tokens)
            allowed = pattern_ref[0, entry] >= 0
            if entry == 0:
                allowed = jnp.logical_and(causal, allowed)
            s = jnp.where(allowed, e_ref[rows, lanes] * (scale * LOG2E), -jnp.inf)
            e_ref[rows, lanes] = s
            top = jnp.max(s, axis=0, keepdims=True)
            peak = top if peak is None else jnp.maximum(peak, top)
        peak = jnp.maximum(peak, FLOOR)
        total = jnp.zeros_like(peak)
        mixed = jnp.zeros_like(peak)
        for d in range(len(entries)):
            rows = slice(d * tokens, (d + 1) * tokens)
            e = jnp.exp2(e_ref[rows, lanes] - peak)
            e_ref[rows, lanes] = e
            total += jnp.sum(e, axis=0, keepdims=True)
            mixed += jnp.sum(e * p_ref[rows, lanes], axis=0, keepdims=True)
        stats_ref[0:1, lanes] = peak
        stats_ref[1:2, lanes] = total
        stats_ref[2:3, lanes] = mixed


def scores_kernel(dims, groups, sources, entries, pattern_ref, q2_ref, u2_ref, *refs):
    nd, kept, pairs, tokens, latent, scale = dims
    early = [refs[3 * g : 3 * g + 3] for g in range(len(groups))]
    ds_ref, rows_ref, grad_ref, tail, s_scr, t_scr, w_scr = refs[-7:]
    key_refs = refs[3 * len(groups) : -7]
    later = [d for d in range(nd) if not any(d in group for group in groups)]
    place_keys(tail, key_refs, [sources[d] for d in later], tokens)
    chosen = [pattern_ref[0, entries[d]] >= 0 for d in later]
    span = lambda p: slice(2 * p * tokens, 2 * (p + 1) * tokens)
    block = lambda k: slice(k * tokens, (k + 1) * tokens)

    def fill(p):
        s_scr[p % 2], t_scr[p % 2] = products(tail, q2_ref, u2_ref, span(p), latent)

    fill(0)
    for p in range(pairs):
        if p + 1 < pairs:
            fill(p + 1)
        lanes = span(p)
        slot = p % 2
        before = [stats_ref[0:1, lanes] for _, _, stats_ref in early]
        peak = functools.reduce(jnp.maximum, before)
        for k in range(len(later)):
            s = jnp.where(chosen[k], s_scr[slot, block(k), :] * (scale * LOG2E), -jnp.inf)
            s_scr[slot, block(k), :] = s
            peak = jnp.maximum(peak, jnp.max(s, axis=0, keepdims=True))
        shrink = [jnp.exp2(b - peak) for b in before]
        total = sum(f * refs3[2][1:2, lanes] for f, refs3 in zip(shrink, early))
        mixed = sum(f * refs3[2][2:3, lanes] for f, refs3 in zip(shrink, early))
        for k in range(len(later)):
            e = jnp.exp2(s_scr[slot, block(k), :] - peak)
            s_scr[slot, block(k), :] = e
            total += jnp.sum(e, axis=0, keepdims=True)
            mixed += jnp.sum(e * t_scr[slot, block(k), :], axis=0, keepdims=True)
        inverse = 1.0 / total
        correction = mixed * inverse
        factors = [f * inverse for f in shrink]
        rows_ref[0:1, lanes] = correction
        for g, factor in enumerate(factors):
            rows_ref[g + 1 : g + 2, lanes] = factor
        for d in range(kept, nd):
            if d in later:
                k = later.index(d)
                e, dp, factor = s_scr[slot, block(k), :], t_scr[slot, block(k), :], inverse
            else:
                g = [d in group for group in groups].index(True)
                source = block(groups[g].index(d))
                e, dp, factor = early[g][0][source, lanes], early[g][1][source, lanes], factors[g]
            w_scr[block(d - kept), lanes] = (e * factor).astype(BF16)
            ds_ref[block(d - kept), lanes] = (e * (factor * scale) * (dp - correction)).astype(BF16)
    main, turned = key_gradient(ds_ref[...], w_scr[...], q2_ref[...], u2_ref[...], latent)
    grad_ref[:, :latent] = main.astype(BF16)
    grad_ref[:, latent:] = turned.astype(BF16)


def kept_gradient(dims, picks, rows_ref, early_refs, q2_ref, u2_ref, ds_ref, w_scr):
    pairs, tokens, latent, scale = dims
    for p in range(pairs):
        lanes = slice(2 * p * tokens, 2 * (p + 1) * tokens)
        correction = rows_ref[0:1, lanes]
        for k, (g, place) in enumerate(picks):
            factor = rows_ref[g + 1 : g + 2, lanes]
            source = slice(place * tokens, (place + 1) * tokens)
            rows = slice(k * tokens, (k + 1) * tokens)
            e, dp = early_refs[2 * g][source, lanes], early_refs[2 * g + 1][source, lanes]
            w_scr[rows, lanes] = (e * factor).astype(BF16)
            ds_ref[rows, lanes] = (e * (factor * scale) * (dp - correction)).astype(BF16)
    return key_gradient(ds_ref[...], w_scr[...], q2_ref[...], u2_ref[...], latent)


def gradient_kernel(dims, picks, rows_ref, q2_ref, u2_ref, *refs):
    *early_refs, grad_ref, ds_ref, w_scr = refs
    latent = dims[2]
    main, turned = kept_gradient(dims, picks, rows_ref, early_refs, q2_ref, u2_ref, ds_ref, w_scr)
    grad_ref[:, :latent] = main
    grad_ref[:, latent:] = turned


def own_kernel(dims, picks, rows_ref, q2_ref, u2_ref, e_ref, p_ref, *refs):
    *met_refs, grad_ref, ds_ref, w_scr = refs
    tokens, latent = dims[1:3]
    main, turned = kept_gradient(
        dims, picks, rows_ref, (e_ref, p_ref), q2_ref, u2_ref, ds_ref, w_scr
    )
    start = jnp.zeros(grad_ref.shape, F32)
    for ref in met_refs:
        is_odd = lax.rem(lax.axis_index("blk"), 2) == 1
        start = jnp.where(is_odd, start, ref[:tokens, :].astype(F32))
    grad_ref[:, :latent] = start[:, :latent] + main
    grad_ref[:, latent:] = start[:, latent:] + turned


def query_kernel(dims, sources, pieces, *refs):
    pairs, tokens, latent, rope = dims
    dq_ref, dr_ref, dq_scr, dr_scr, ds_ref, keys_ref, sems = refs[-7:]
    place_keys(keys_ref, refs[pieces:-7], sources, tokens)
    at = 0
    for ref in refs[:pieces]:
        ds_ref[at : at + ref.shape[0], :] = ref[...]
        at += ref.shape[0]
    tn = (((0,), (0,)), ((), ()))
    lane = lax.broadcasted_iota(jnp.int32, (tokens, 2 * rope), 1)
    copies = []
    for p in range(pairs):
        lanes = slice(2 * p * tokens, 2 * (p + 1) * tokens)
        dq = lax.dot_general(ds_ref[:, lanes], keys_ref[...], tn, preferred_element_type=F32)
        even, odd = dq[:tokens], dq[tokens:]
        out = 2 * p * latent
        dq_scr[:, out : out + latent] = even[:, :latent].astype(BF16)
        dq_scr[:, out + latent : out + 2 * latent] = odd[:, :latent].astype(BF16)
        turned = jnp.where(lane < rope, even[:, latent:], odd[:, latent:])
        dr_scr[:, 2 * p * rope : 2 * (p + 1) * rope] = turned.astype(BF16)
        cols = slice(out, out + 2 * latent)
        copies.append(pltpu.make_async_copy(dq_scr.at[:, cols], dq_ref.at[:, cols], sems.at[p]))
        copies[-1].start()
    copies.append(pltpu.make_async_copy(dr_scr, dr_ref, sems.at[pairs]))
    copies[-1].start()
    for copy in copies:
        copy.wait()


def per_device(query_latent, query_rotary, upstream, latent, key_rotary, pattern):
    blocks = lax.axis_size("blk")
    spacing = spacing_list(blocks)
    nd = len(spacing)
    inner = lax.axis_size("inner")
    tokens = query_latent.shape[0]
    shard, width = latent.shape
    rope = key_rotary.shape[1]
    heads = query_latent.shape[1] // width
    pairs = heads // 2
    wide = width + 2 * rope
    depth = nd * tokens
    rows = heads * tokens
    scale = (NOPE + rope) ** (-0.5)
    paired = spacing == [0, 1, 2, 3, 4] and blocks % 2 == 0

    hbm = pl.BlockSpec(memory_space=pltpu.HBM)
    vmem = pl.BlockSpec(memory_space=pltpu.VMEM)
    smem = pl.BlockSpec(memory_space=pltpu.SMEM)
    params = pltpu.CompilerParams(vmem_limit_bytes=VMEM)

    def staged(lanes, array, *ropes):
        return pl.pallas_call(
            functools.partial(stage_kernel, (heads, tokens, width, rope)),
            in_specs=[hbm] + [vmem] * len(ropes),
            out_specs=vmem,
            out_shape=jax.ShapeDtypeStruct((rows, lanes), BF16),
            scratch_shapes=[pltpu.SemaphoreType.DMA((heads,))],
            cost_estimate=pl.CostEstimate(
                flops=rows * lanes * width, bytes_accessed=4 * rows * lanes, transcendentals=0
            ),
            compiler_params=params,
        )(array, *ropes)

    q2 = staged(wide, query_latent, query_rotary)
    own = jnp.concatenate([latent, key_rotary, key_rotary], axis=1)
    gathered = [own] + [rotated(own, "inner", k) for k in range(1, inner)]
    gathered = lax.optimization_barrier(gathered)
    near = jnp.concatenate(gathered, axis=0)
    u2 = staged(width, upstream)
    if paired:
        order = [4, 2, 0, 1, 3]
        kept = 3
        groups = [[1, 2], [0, 3]]
        two = rotated(near, "blk", 2)
        four = rotated(near, "blk", 4)
        near_met = swapped(near)
        two, q2, u2 = lax.optimization_barrier((two, q2, u2))
        two_met = swapped(two)
        sources = [(2,), (1,), (0,), (4, 3), (5, 4)]
    else:
        order = spacing
        kept = 1
        groups = [[0]]
        sources = [(d,) for d in range(nd)]
    sent = nd - kept
    entries = [spacing.index(d) for d in order]
    behind = depth - sum(len(group) for group in groups) * tokens

    def early_scores(group, key_arrays, sources):
        ahead = len(group) * tokens
        return pl.pallas_call(
            functools.partial(
                early_kernel,
                (pairs, tokens, shard, width, scale),
                sources,
                [entries[d] for d in group],
            ),
            in_specs=[smem] + [vmem] * (2 + len(key_arrays)),
            out_specs=[vmem] * 3,
            out_shape=[
                jax.ShapeDtypeStruct((ahead, rows), F32),
                jax.ShapeDtypeStruct((ahead, rows), F32),
                jax.ShapeDtypeStruct((8, rows), F32),
            ],
            scratch_shapes=[pltpu.VMEM((ahead, wide), BF16)],
            cost_estimate=pl.CostEstimate(
                flops=2 * rows * ahead * (wide + width),
                bytes_accessed=8 * rows * ahead,
                transcendentals=rows * ahead,
            ),
            compiler_params=params,
        )(pattern, q2, u2, *key_arrays)

    if paired:
        first = early_scores(groups[0], [two, near], [(0,), (1,)])
        four, first = lax.optimization_barrier((four, first))
        four_met = swapped(four)
        second = early_scores(groups[1], [four, near_met, two_met], [(0,), (2, 1)])
        early = [*first, *second]
        key_arrays = [near, two, four, near_met, two_met, four_met]
    else:
        early = early_scores(groups[0], [near], [(0,)])
        key_arrays = [near] + [rotated(near, "blk", d) for d in spacing[1:]]
    queries = (q2, u2)

    ds_sent, row_values, grads = pl.pallas_call(
        functools.partial(
            scores_kernel, (nd, kept, pairs, tokens, width, scale), groups, sources, entries
        ),
        in_specs=[smem] + [vmem] * (2 + len(early) + len(key_arrays)),
        out_specs=[vmem] * 3,
        out_shape=[
            jax.ShapeDtypeStruct((sent * tokens, rows), BF16),
            jax.ShapeDtypeStruct((8, rows), F32),
            jax.ShapeDtypeStruct((sent * tokens, wide), BF16),
        ],
        scratch_shapes=[
            pltpu.VMEM((behind, wide), BF16),
            pltpu.VMEM((2, behind, 2 * tokens), F32),
            pltpu.VMEM((2, behind, 2 * tokens), F32),
            pltpu.VMEM((sent * tokens, rows), BF16),
        ],
        cost_estimate=pl.CostEstimate(
            flops=2 * rows * (behind + sent * tokens) * (wide + width),
            bytes_accessed=8 * rows * depth,
            transcendentals=rows * behind,
        ),
        compiler_params=params,
        name="scores",
    )(pattern, *queries, *early, *key_arrays)

    part_shapes = [
        jax.ShapeDtypeStruct((shard, wide), F32 if k == 0 else BF16) for k in range(inner)
    ]
    wide_dims = (pairs, tokens, width, scale)
    exponents = [x for k, x in enumerate(early) if k % 3 < 2]
    place_of = lambda d: [(g, group.index(d)) for g, group in enumerate(groups) if d in group][0]
    if paired:
        met = swapped(grads)
        late_rows = (kept - 1) * tokens
        late, ds_late = pl.pallas_call(
            functools.partial(gradient_kernel, wide_dims, [place_of(d) for d in range(kept - 1)]),
            out_shape=[
                jax.ShapeDtypeStruct((late_rows, wide), F32),
                jax.ShapeDtypeStruct((late_rows, rows), BF16),
            ],
            scratch_shapes=[pltpu.VMEM((late_rows, rows), BF16)],
            cost_estimate=pl.CostEstimate(
                flops=2 * rows * late_rows * (wide + width),
                bytes_accessed=4 * rows * wide,
                transcendentals=0,
            ),
            compiler_params=params,
            name="late_gradients",
        )(row_values, *queries, *exponents)
        to_two, *four_parts = pl.pallas_call(
            merge_kernel,
            out_shape=[jax.ShapeDtypeStruct((tokens, wide), BF16)] + part_shapes,
            compiler_params=params,
            name="merge",
        )(late, met)
        back = [rotated(to_two, "blk", -2)]
        four_moved = [rotated(four_parts[k], "inner", -k) for k in range(1, inner)]
        four_shard = pl.pallas_call(
            sum_kernel,
            out_shape=jax.ShapeDtypeStruct((shard, wide), BF16),
            compiler_params=params,
            name="sum_four",
        )(four_parts[0], *four_moved)
        shards_back = [rotated(four_shard, "blk", -4)]
        handed = [met]
        ds_pieces = [ds_late]
    else:
        back = [
            rotated(grads[k * tokens : (k + 1) * tokens], "blk", -d)
            for k, d in enumerate(spacing[1:])
        ]
        handed = []
        ds_pieces = []
        shards_back = []

    own_grad, ds_own = pl.pallas_call(
        functools.partial(own_kernel, wide_dims, [place_of(kept - 1)]),
        out_shape=[
            jax.ShapeDtypeStruct((tokens, wide), F32),
            jax.ShapeDtypeStruct((tokens, rows), BF16),
        ],
        scratch_shapes=[pltpu.VMEM((tokens, rows), BF16)],
        cost_estimate=pl.CostEstimate(
            flops=2 * rows * tokens * (wide + width),
            bytes_accessed=2 * rows * wide,
            transcendentals=0,
        ),
        compiler_params=params,
        name="own_gradients",
    )(row_values, *queries, *exponents[:2], *handed)
    ds_pieces = ds_pieces + [ds_own, ds_sent]

    query_cotangent, rotary_cotangent = pl.pallas_call(
        functools.partial(
            query_kernel, (pairs, tokens, width, rope), sources, len(ds_pieces)
        ),
        in_specs=[vmem] * (len(ds_pieces) + len(key_arrays)),
        out_specs=[hbm] * 2,
        out_shape=[
            jax.ShapeDtypeStruct(query_latent.shape, BF16),
            jax.ShapeDtypeStruct(query_rotary.shape, BF16),
        ],
        scratch_shapes=[
            pltpu.VMEM(query_latent.shape, BF16),
            pltpu.VMEM(query_rotary.shape, BF16),
            pltpu.VMEM((depth, rows), BF16),
            pltpu.VMEM((depth, wide), BF16),
            pltpu.SemaphoreType.DMA((pairs + 1,)),
        ],
        cost_estimate=pl.CostEstimate(
            flops=2 * rows * depth * wide,
            bytes_accessed=2 * rows * (wide + depth),
            transcendentals=0,
        ),
        compiler_params=params,
        name="query_cotangents",
    )(*ds_pieces, *key_arrays)

    parts = pl.pallas_call(
        functools.partial(total_kernel, len(back)),
        out_shape=part_shapes,
        compiler_params=params,
        name="total",
    )(own_grad, *back)
    moved = [rotated(parts[k], "inner", -k) for k in range(1, inner)]

    latent_cotangent, positional_cotangent = pl.pallas_call(
        functools.partial(finish_kernel, (width, rope)),
        out_shape=[
            jax.ShapeDtypeStruct((shard, width), F32),
            jax.ShapeDtypeStruct((shard, rope), F32),
        ],
        compiler_params=params,
        name="finish",
    )(parts[0], *moved, *shards_back)
    return (query_cotangent, rotary_cotangent, latent_cotangent, positional_cotangent)


def solution(mesh):
    in_specs = (
        P("blk", "inner"),
        P("blk", "inner"),
        P("blk", "inner"),
        P(("blk", "inner"), None),
        P(("blk", "inner"), None),
        P("blk", None),
    )
    out_specs = (
        P("blk", "inner"),
        P("blk", "inner"),
        P(("blk", "inner"), None),
        P(("blk", "inner"), None),
    )

    return jax.shard_map(per_device, mesh=mesh, in_specs=in_specs, out_specs=out_specs, check_vma=False)
```
